128 devices in a mesh: row: 16 (over x, z), col: 8 (over y, core).
Axes of the slice: x: 4, y: 4, z: 4, core: 2. Of those that a mesh axis runs over, the one named last changes fastest.
Arguments:
- coeffs: bfloat16 [4096, 128, 128], P(('row', 'col')), as said below
- tiles: int32 [4096, 1], replicated, may hold values from 0 to 7; in each aligned block of 32 rows (0 to 31, 32 to 63, ...) at most 5 rows name the same one
- primal: bfloat16 [1024, 1024], replicated, as said below
- dual_inverse: bfloat16 [1024, 1024], replicated, as said below
Outputs:
- schur: float32 [4096, 4096], P('row', 'col')
The draws below stay inside these ranges and needn't reach their ends.
Inputs may be any that keep to these rules, and one draw needn't show every extreme that they name: `tiles`: within each aligned block of 32 constraints (the constraints of one device) no tile is named more than 5 times, a bound that some block reaches. Each coeffs[i] is symmetric. `primal`: Symmetric. `dual_inverse`: Symmetric.
All inputs are finite; a program needn't handle non-finite values.
Results may differ from the reference program's by a relative error of at most 0.0022.
Values may be sent and summed in bfloat16 or wider, within the bound.
No kernel may reach another device: no remote copies, remote signals or barrier semaphores. Data moves between devices by JAX's collectives and lax.ppermute only.
A program may use at most 128 MiB of HBM per device.

```python
import math
import jax
import jax.numpy as jnp
import numpy as np
from jax import lax

N = 1024
K = 128
CDEV = 32
NT = 8
MOST = 5
M = 4096


def symmetric_block(key, salt):
    value_key = jax.random.fold_in(key, salt)
    diagonal_key = jax.random.fold_in(key, salt + 1)
    raw_values = jnp.clip(jax.random.normal(value_key, (N, N), jnp.float32), -6.0, 6.0)
    matrix = (raw_values + raw_values.T) * 0.5 ** 0.5 / K ** 0.5
    matrix = matrix + jnp.diag(jax.random.uniform(diagonal_key, (N,), jnp.float32, 0.5, 1.5))
    return matrix.astype(jnp.bfloat16)


def draw_primal(key, part):
    return symmetric_block(key, 101)


def draw_dual_inverse(key, part):
    return symmetric_block(key, 211)


def draw_coeffs(key, part):
    value_key = jax.random.fold_in(key, 307)
    raw_values = jnp.clip(jax.random.normal(value_key, (M, K, K), jnp.float32), -6.0, 6.0)
    symmetric = (raw_values + jnp.swapaxes(raw_values, 1, 2)) * 0.5 ** 0.5 / K ** 0.5
    return symmetric.astype(jnp.bfloat16)


def shared_out(own_key, own, number, rows, count, top, bound, skew):
    ranking = jax.random.permutation(own_key, count)
    heavy_load, ordinary = shares(count, rows * top, bound, skew, True), shares(count, rows * top, bound, skew, False)
    places = jnp.arange(count)

    def named(tallies, offset_by):
        used = int((tallies > 0).sum())
        fixed = max(1, used // 4)
        passed = fixed + (places - fixed + offset_by * (used - fixed)) % max(1, count - fixed)
        return jnp.zeros((count,), jnp.int32).at[ranking[jnp.where(places < fixed, places, passed)]].set(jnp.asarray(tallies, jnp.int32))

    tallies = jnp.where(number % 4 == 0, named(heavy_load, number // 4), named(ordinary, number - number // 4 - 1))
    mixed = jax.random.permutation(jax.random.fold_in(own, 3), count)
    giver, receiver = mixed[0:count // 2 * 2:2], mixed[1:count // 2 * 2:2]
    slack = jnp.minimum(tallies[giver] - 1, bound - tallies[receiver]) // 2
    slack = jnp.where((giver == ranking[0]) | (receiver == ranking[0]) | (tallies[receiver] == 0), 0, jnp.maximum(slack, 0))
    passed = jax.random.randint(jax.random.fold_in(own, 4), (count // 2,), 0, 1 << 20) % (slack + 1)
    tallies = tallies.at[giver].add(-passed).at[receiver].add(passed)
    members = jnp.searchsorted(jnp.cumsum(tallies), jnp.arange(rows * top), side="right").astype(jnp.int32)
    table = members.reshape(top, rows).T
    table = table[jax.random.permutation(jax.random.fold_in(own, 1), rows)]
    offset_by = jax.random.randint(jax.random.fold_in(own, 2), (rows, 1), 0, top)
    return jnp.take_along_axis(table, (jnp.arange(top)[None, :] + offset_by) % top, axis=1)


def shares(amount, total, limit, skew, full):
    loads = [(1 << 20) // math.isqrt(grade ** skew) + 1 for grade in range(1, amount + 1)]
    largest = limit if full else min(limit, max(-(-total // amount), total * loads[0] // sum(loads)))
    least = 1 if total - largest >= amount - 1 else 0
    given, spare = [largest] + [least] * (amount - 1), total - largest - least * (amount - 1)
    while spare > 0:
        free = [i for i in range(1, amount) if given[i] < largest] or [i for i in range(1, amount) if given[i] < limit]
        mass, remaining = sum([loads[i] for i in free]), spare
        for i in free:
            more = min(limit - given[i], max(1, remaining * loads[i] // mass), spare)
            given[i] = given[i] + more
            spare = spare - more
    return np.array(given)


def setup_inputs(seed: int = 0) -> dict:
    splits = jax.random.split(jax.random.key(seed), 5)
    coeffs = draw_coeffs(jax.random.fold_in(splits[4], 71), 0)
    tiles_keys = jax.random.split(jax.random.fold_in(splits[1], 1), M // CDEV)
    tiles_turns = jax.random.permutation(jax.random.fold_in(splits[1], 3), M // CDEV)
    tiles = jax.vmap(lambda own, number: shared_out(jax.random.fold_in(splits[1], 2), own, number, CDEV, NT, 1, MOST, 2))(tiles_keys, tiles_turns).reshape((M, 1))
    primal = draw_primal(jax.random.fold_in(splits[4], 71), 0)
    dual_inverse = draw_dual_inverse(jax.random.fold_in(splits[4], 71), 0)
    return dict(coeffs=coeffs, tiles=tiles, primal=primal, dual_inverse=dual_inverse)


def slot_ranks(tile_group, first_tile, tile_width):
    labels = first_tile + jnp.arange(tile_width, dtype=jnp.int32)
    member = (tile_group[:, :, None] == labels[None, None, :]).astype(jnp.int32)
    before = jnp.cumsum(member, axis=1) - member
    return member, jnp.sum(before * member, axis=2)


def reference(coeffs, tiles, primal, dual_inverse):
    tile_count = N // K
    total = coeffs.shape[0]
    blocks = total // CDEV
    tile_area = K * K
    tile_ids = tiles[:, 0].astype(jnp.int32)
    member, ordinal = slot_ranks(tile_ids.reshape(blocks, CDEV), 0, tile_count)
    levels = jnp.arange(MOST, dtype=jnp.int32)
    chosen = member[:, :, :, None] * (ordinal[:, :, None, None] == levels[None, None, None, :]).astype(jnp.int32)
    offsets = jnp.arange(CDEV, dtype=jnp.int32)
    source = jnp.sum(chosen * offsets[None, :, None, None], axis=1)
    filled = jnp.sum(chosen, axis=1)
    anchor = (jnp.arange(blocks, dtype=jnp.int32)[:, None, None] * CDEV + source).reshape(-1).astype(jnp.int32)
    flat_coeffs = coeffs.reshape(total, tile_area).astype(jnp.float32)
    slot_rows = jnp.take(flat_coeffs, anchor, axis=0) * filled.reshape(-1, 1).astype(jnp.float32)
    slot_rows = slot_rows.reshape(blocks, tile_count, MOST, tile_area)
    position = (jnp.arange(blocks, dtype=jnp.int32)[:, None] * (tile_count * MOST)
                + tile_ids.reshape(blocks, CDEV) * MOST + ordinal).reshape(-1).astype(jnp.int32)
    primal_tiles = primal.reshape(tile_count, K, tile_count, K).astype(jnp.float32)
    dual_tiles = dual_inverse.reshape(tile_count, K, tile_count, K).astype(jnp.float32)
    block_rows = math.gcd(total, 64)

    def one_block(first_row):
        row_coeffs = lax.dynamic_slice_in_dim(coeffs, first_row, block_rows, 0).astype(jnp.float32)
        row_tiles = lax.dynamic_slice_in_dim(tile_ids, first_row, block_rows, 0)
        primal_pick = jnp.take(primal_tiles, row_tiles, axis=0)
        product_tile = jnp.einsum("iab,ibuc->iuac", row_coeffs, primal_pick).astype(jnp.bfloat16)
        dual_pick = jnp.take(dual_tiles, row_tiles, axis=2)
        reduced = jnp.einsum("iuba,ucib->iuac", product_tile.astype(jnp.float32), dual_pick).astype(jnp.bfloat16)
        reduced = reduced.reshape(block_rows, tile_count, tile_area).astype(jnp.float32)
        values = jnp.einsum("iux,suqx->isuq", reduced, slot_rows).reshape(block_rows, -1)
        return jnp.take(values, position, axis=1)

    starts = jnp.arange(0, total, block_rows, dtype=jnp.int32)
    return lax.map(one_block, starts).reshape(total, total)
```

```python
import jax
import jax.numpy as jnp
import numpy as np
from jax import lax
from jax.experimental import pallas as pl
from jax.experimental.pallas import tpu as pltpu
from jax.sharding import Mesh
from jax.sharding import PartitionSpec as P


MOST = 5
K = 128
H = 64
FOLD = H + 1
WIDTH = FOLD * K
UNIT = 8 * MOST
LINE = ("y", "core")
PLANE = ("x", "z")
ALL = ("x", "z", "y", "core")

HOPS = (
    ((1, 0), (0, 0)),
    ((0, 3), (0, 0)),
    ((3, 1), (0, 0)),
    ((2, 0), (1, 0)),
    ((0, 2), (0, 3)),
    ((2, 1), (3, 1)),
    ((3, 2), (3, 1)),
    ((3, 3), (0, 3)),
    ((2, 2), (2, 1)),
)


def negated(d):
    return ((-d[0]) % 4, (-d[1]) % 4)


FORMED = ((0, 0),) + tuple(d for d, _ in HOPS)


def plane_shift(x, shift):
    pairs = []
    for a in range(4):
        for b in range(4):
            pairs.append((a * 4 + b, (a + shift[0]) % 4 * 4 + (b + shift[1]) % 4))
    return lax.ppermute(x, PLANE, pairs)


def ring_shift(x, axis, size, shift):
    return lax.ppermute(x, axis, [(a, (a + shift) % size) for a in range(size)])


def folded(square, half_diagonal):
    top, bottom = square[:H], square[H:]
    row = lax.broadcasted_iota(jnp.int32, (H, K), 0)
    lane = lax.broadcasted_iota(jnp.int32, (H, K), 1)
    turned = pltpu.roll(bottom, H, 1)
    kept = jnp.where(jnp.logical_and(lane < H, row > lane), turned, top)
    last = jnp.sum(jnp.where(lane == row + H, bottom, 0.0), axis=0, keepdims=True)
    if half_diagonal:
        kept = kept * jnp.where(row == lane, 0.5, 1.0)
        last = last * 0.5
    return kept, last


PIECE = 2 * MOST * H + 16


def fold_kernel(table, own_ref, other_ref, *out_refs):
    for k in range(4):
        out = out_refs[k]
        out[2 * MOST * H :, :] = jnp.zeros((16, K), out.dtype)

        lasts = []
        for s in range(2 * MOST):
            at = table[k * 2 * MOST + s]
            place = jnp.maximum(at, 0)
            within = lax.rem(place, 32)
            scale = (at >= 0).astype(jnp.float32)
            pick = (place >= 32).astype(jnp.float32)
            own = own_ref[within].astype(jnp.float32)
            other = other_ref[within].astype(jnp.float32)
            square = jnp.where(pick > 0.5, other, own)
            square = jnp.where(scale > 0.5, square, 0.0)
            kept, last = folded(square, False)
            out[s * H : (s + 1) * H, :] = kept.astype(out.dtype)
            lasts.append(last)
        lasts.append(jnp.zeros((6, K), jnp.float32))
        out[2 * MOST * H :, :] = jnp.concatenate(lasts, axis=0).astype(out.dtype)


def fold_call(table, own, other):
    whole = pl.BlockSpec(memory_space=pltpu.VMEM)
    return pl.pallas_call(
        fold_kernel,
        out_shape=[jax.ShapeDtypeStruct((PIECE, K), jnp.bfloat16)] * 4,
        in_specs=[pl.BlockSpec(memory_space=pltpu.SMEM), whole, whole],
        out_specs=[whole] * 4,
        name="fold",
    )(table, own, other)


def unit_kernel(*refs):
    pieces, out, turn = refs[:4], refs[4], refs[5]
    for k in range(4):
        for s in range(2 * MOST):
            slot = k * 2 * MOST + s
            turn[pl.ds(slot, H, stride=UNIT), :] = pieces[k][s * H : (s + 1) * H, :].astype(jnp.float32)
        first = H * UNIT + k * 2 * MOST
        turn[first : first + 2 * MOST, :] = pieces[k][2 * MOST * H :, :].astype(jnp.float32)[: 2 * MOST]
    for a in range(FOLD):
        out[:, a * K : (a + 1) * K] = turn[a * UNIT : (a + 1) * UNIT, :].astype(out.dtype)


def unit_call(pieces):
    whole = pl.BlockSpec(memory_space=pltpu.VMEM)
    return pl.pallas_call(
        unit_kernel,
        out_shape=jax.ShapeDtypeStruct((UNIT, WIDTH), jnp.bfloat16),
        in_specs=[whole] * 4,
        out_specs=whole,
        scratch_shapes=[pltpu.VMEM((FOLD * UNIT, K), jnp.float32)],
        name="unit",
    )(*pieces)


STRIDE = 40


def reduce_kernel(block, ids, coeffs, right, left, *refs):
    out, turn = refs[-2], refs[-1]

    def four(n, carry):
        for m in range(4):
            i = n * 4 + m
            t = ids[i]
            wide = jnp.dot(coeffs[i], right[t], preferred_element_type=jnp.float32)
            wide = wide.astype(jnp.bfloat16)
            tall = jnp.concatenate([wide[:, :K], wide[:, K:]], axis=0)
            both = jnp.dot(left[t], tall, preferred_element_type=jnp.float32)
            kept, last = folded(both, True)
            turn[pl.ds(i, H, stride=STRIDE), :] = kept
            turn[pl.ds(H * STRIDE + i, 1), :] = last
        return carry

    lax.fori_loop(0, 8, four, 0)
    for a in range(FOLD):
        out[:, a * K : (a + 1) * K] = turn[a * STRIDE : a * STRIDE + 32, :].astype(out.dtype)


def reduce_call(block, ids, coeffs, right, left, total):
    def fixed3(i, block, ids):
        return (0, 0, 0)

    specs = [
        pl.BlockSpec((32, K, K), fixed3),
        pl.BlockSpec((8, K, 2 * K), fixed3),
        pl.BlockSpec((8, K, 2 * K), fixed3),
    ]
    args = [coeffs, right, left]
    aliases = {}
    if total is not None:
        specs.append(pl.BlockSpec(memory_space=pl.ANY))
        args.append(total)
        aliases = {5: 0}
    return pl.pallas_call(
        reduce_kernel,
        out_shape=jax.ShapeDtypeStruct((256, WIDTH), jnp.bfloat16),
        grid_spec=pltpu.PrefetchScalarGridSpec(
            num_scalar_prefetch=2,
            grid=(1,),
            in_specs=specs,
            out_specs=pl.BlockSpec((32, WIDTH), lambda i, block, ids: (block[0], 0)),
            scratch_shapes=[pltpu.VMEM((FOLD * STRIDE, K), jnp.float32)],
        ),
        input_output_aliases=aliases,
        name="reduced",
    )(block, ids, *args)


def final_kernel(flags, places_ref, landed, out):
    for g in range(2):
        places = places_ref[:, g : g + 1]
        slots = lax.broadcasted_iota(jnp.int32, (256, 8 * UNIT), 1)
        hot = (slots == places).astype(jnp.bfloat16)
        values = jnp.concatenate([landed[c, g] for c in range(8)], axis=0)
        high = values.astype(jnp.bfloat16)
        rest = values - high.astype(jnp.float32)
        low = rest.astype(jnp.bfloat16)
        picked = jnp.dot(hot, high, preferred_element_type=jnp.float32)
        picked = picked + jnp.dot(hot, low, preferred_element_type=jnp.float32)
        turned = flags[g] > 0

        @pl.when(turned)
        def _():
            out[:, g * 256 : (g + 1) * 256] = picked

        @pl.when(jnp.logical_not(turned))
        def _():
            out[:, g * 256 : (g + 1) * 256] = picked.T


def final_call(flags, places, landed):
    whole = pl.BlockSpec(memory_space=pltpu.VMEM)
    return pl.pallas_call(
        final_kernel,
        out_shape=jax.ShapeDtypeStruct((256, 512), jnp.float32),
        in_specs=[pl.BlockSpec(memory_space=pltpu.SMEM), whole, whole],
        out_specs=whole,
        name="final",
    )(flags, places, landed)


def shards(coeffs, tiles, primal, dual_inverse):
    x, z = lax.axis_index("x"), lax.axis_index("z")
    y, core = lax.axis_index("y"), lax.axis_index("core")
    line = x * 4 + z
    tile = y * 2 + core
    ids = tiles.reshape(128, 32)
    earlier = jnp.tril(jnp.ones((32, 32), jnp.int32), -1)
    same = (ids[:, :, None] == ids[:, None, :]).astype(jnp.int32)
    ordinal = jnp.sum(same * earlier[None], axis=2)

    block = jnp.arange(128, dtype=jnp.int32)[:, None] % 8
    step = (ids // 2 - block // 2) % 4
    place = ids * UNIT + step * 2 * MOST + (block % 2) * MOST + ordinal
    place = place.reshape(16, 256)

    chip = (line * 8 + y * 2).astype(jnp.int32)
    chip_ids = lax.dynamic_slice_in_dim(ids, chip, 2, 0)
    chip_ordinal = lax.dynamic_slice_in_dim(ordinal, chip, 2, 0)
    wanted = (y + jnp.arange(4, dtype=jnp.int32)) % 4 * 2 + core
    levels = jnp.arange(MOST, dtype=jnp.int32)
    match = jnp.logical_and(
        chip_ids[None, :, None, :] == wanted[:, None, None, None],
        chip_ordinal[None, :, None, :] == levels[None, None, :, None],
    )
    halves = jnp.arange(2, dtype=jnp.int32)
    source = jnp.where(halves == core, 0, 32)[:, None] + jnp.arange(32, dtype=jnp.int32)[None, :]
    table = jnp.sum(jnp.where(match, source[None, :, None, :] + 1, 0), axis=3) - 1
    table = table.reshape(UNIT).astype(jnp.int32)

    other = ring_shift(coeffs, "core", 2, 1)
    pieces = fold_call(table, coeffs, other)
    routed = [pieces[0]] + [ring_shift(pieces[k], "y", 4, k) for k in (1, 2, 3)]
    units = {(0, 0): unit_call(routed)}

    line_ids = lax.dynamic_slice_in_dim(ids, line * 8, 8, 0)
    rows_u = lax.dynamic_slice_in_dim(primal, tile * K, K, 0).reshape(K, 8, K)
    rows_v = lax.dynamic_slice_in_dim(dual_inverse, tile * K, K, 0).reshape(K, 8, K)
    left = jnp.concatenate([rows_u, rows_v], axis=2).transpose(1, 0, 2)
    cols_u = lax.dynamic_slice_in_dim(primal, tile * K, K, 1).reshape(8, K, K)
    cols_v = lax.dynamic_slice_in_dim(dual_inverse, tile * K, K, 1).reshape(8, K, K)
    right = jnp.concatenate([cols_v, cols_u], axis=2)

    def formed(total, block_y, block_core, values):
        at = (block_y * 2 + block_core).astype(jnp.int32)
        own_ids = lax.dynamic_slice_in_dim(line_ids, at, 1, 0).reshape(32)
        return reduce_call(at.reshape(1), own_ids, values, right, left, total)

    total = formed(None, y, core, coeffs)
    total = formed(total, y, 1 - core, other)
    for k in (1, 3, 2):
        near = ring_shift(coeffs, "y", 4, k)
        total = formed(total, (y - k) % 4, core, near)
        far = ring_shift(near, "core", 2, 1)
        total = formed(total, (y - k) % 4, 1 - core, far)

    for d, parent in HOPS:
        shift = ((d[0] - parent[0]) % 4, (d[1] - parent[1]) % 4)
        units[d] = plane_shift(units[parent], shift)

    found = {}
    for d in FORMED:
        found[d] = lax.dot_general(
            units[d], total, (((1,), (1,)), ((), ())), preferred_element_type=jnp.float32
        )
    for d in FORMED:
        if negated(d) not in FORMED:
            found[negated(d)] = plane_shift(found[d], negated(d))

    stacked = jnp.stack([found[(a, b)] for a in range(4) for b in range(4)])
    group = jnp.arange(16, dtype=jnp.int32)
    apart = (x - group // 4) % 4 * 4 + (z - group % 4) % 4
    ordered = jnp.take(stacked, apart, axis=0)
    landed = lax.all_to_all(ordered.reshape(8, 2, UNIT, 256), LINE, 0, 0, tiled=True)

    flips = np.array([0 if (a, b) in FORMED else 1 for a in range(4) for b in range(4)], np.int32)
    mine = tile * 2 + jnp.arange(2, dtype=jnp.int32)
    apart_mine = (x - mine // 4) % 4 * 4 + (z - mine % 4) % 4
    flags = jnp.take(jnp.asarray(flips), apart_mine)
    row_place = lax.dynamic_slice_in_dim(place, line, 1, 0)
    col_place = lax.dynamic_slice_in_dim(place, tile * 2, 2, 0)
    places = jnp.where(flags[:, None] > 0, row_place, col_place)
    return final_call(flags, places.T, landed)


def solution(mesh):
    finer = Mesh(mesh.devices.reshape(4, 4, 4, 2), ALL)
    in_specs = (P(ALL, None, None), P(), P(), P())
    out_specs = P(PLANE, LINE)
    return jax.shard_map(
        shards, mesh=finer, in_specs=in_specs, out_specs=out_specs, check_vma=False
    )
```

```python
import functools

import jax
import jax.numpy as jnp
import numpy as np
from jax import lax
from jax.experimental import pallas as pl
from jax.experimental.pallas import tpu as pltpu
from jax.sharding import Mesh
from jax.sharding import PartitionSpec as P


MOST = 5
K = 128
H = 64
FOLD = H + 1
WIDTH = FOLD * K
UNIT = 8 * MOST
PIECE = MOST * H + 16
LINE = ("y", "core")
PLANE = ("x", "z")
ALL = ("x", "z", "y", "core")
NT = (((1,), (1,)), ((), ()))
VMEM = pl.BlockSpec(memory_space=pltpu.VMEM)
SMEM = pl.BlockSpec(memory_space=pltpu.SMEM)
ANY = pl.BlockSpec(memory_space=pl.ANY)

FIRST = (((1, 0), (0, 0)), ((0, 3), (0, 0)), ((3, 1), (0, 0)))
SECOND = (((2, 1), (3, 1)), ((3, 2), (3, 1)), ((2, 0), (1, 0)), ((0, 2), (0, 3)), ((3, 3), (0, 3)))
THIRD = (((2, 2), (2, 1)),)
EARLY = ((0, 0),) + tuple(d for d, _ in FIRST + SECOND)
LATE = tuple(d for d, _ in THIRD)
FORMED = EARLY + LATE


def negated(d):
    return ((-d[0]) % 4, (-d[1]) % 4)


TURNED = tuple(negated(d) for d in FORMED if negated(d) not in FORMED)


def plane_shift(x, shift):
    pairs = []
    for a in range(4):
        for b in range(4):
            pairs.append((a * 4 + b, (a + shift[0]) % 4 * 4 + (b + shift[1]) % 4))
    return lax.ppermute(x, PLANE, pairs)


def line_shift(x, shift, swap):
    pairs = []
    for a in range(4):
        for b in range(2):
            pairs.append((a * 2 + b, (a + shift) % 4 * 2 + (b + swap) % 2))
    return lax.ppermute(x, LINE, pairs)


def folded(square, half_diagonal):
    top, bottom = square[:H], square[H:]
    row = lax.broadcasted_iota(jnp.int32, (H, K), 0)
    lane = lax.broadcasted_iota(jnp.int32, (H, K), 1)
    turned = pltpu.roll(bottom, H, 1)
    kept = jnp.where(jnp.logical_and(lane < H, row > lane), turned, top)
    last = jnp.sum(jnp.where(lane == row + H, bottom, 0.0), axis=0, keepdims=True)
    if half_diagonal:
        kept = kept * jnp.where(row == lane, 0.5, 1.0)
        last = last * 0.5
    return kept, last


def fold_kernel(where, tiles, own_ref, *refs):
    outs, held, lasts, counts = refs[:8], refs[8], refs[9], refs[10]
    held[...] = jnp.zeros(held.shape, held.dtype)
    lasts[...] = jnp.zeros(lasts.shape, lasts.dtype)
    for k in range(8):
        counts[k] = 0
    y, core = where[1], where[2]
    mine = where[0] * 256 + y * 64 + core * 32

    def four(n, carry):
        for m in range(8):
            i = n * 8 + m
            t = tiles[mine + i]
            order = counts[t]
            counts[t] = order + 1
            goal = lax.rem(t // 2 - y + 4, 4) * 2 + lax.rem(t + core, 2)
            kept, last = folded(own_ref[i].astype(jnp.float32), False)
            row = pl.multiple_of(goal * PIECE + order * H, 16)
            held[pl.ds(row, H), :] = kept.astype(held.dtype)
            lasts[pl.ds(goal * 16 + order, 1), :] = last
        return carry

    lax.fori_loop(0, 4, four, 0)
    for k in range(8):
        outs[k][: MOST * H, :] = held[k * PIECE : k * PIECE + MOST * H, :]
        outs[k][MOST * H :, :] = lasts[k * 16 : (k + 1) * 16, :].astype(held.dtype)


def fold_call(where, tiles, own):
    return pl.pallas_call(
        fold_kernel,
        out_shape=[jax.ShapeDtypeStruct((PIECE, K), jnp.bfloat16)] * 8,
        in_specs=[SMEM, SMEM, VMEM],
        out_specs=[VMEM] * 8,
        scratch_shapes=[
            pltpu.VMEM((8 * PIECE, K), jnp.bfloat16),
            pltpu.VMEM((8 * 16, K), jnp.float32),
            pltpu.SMEM((8,), jnp.int32),
        ],
        name="fold",
    )(where, tiles, own)


def unit_kernel(*refs):
    pieces, out, turn = refs[:8], refs[8], refs[9]
    for k in range(8):
        for s in range(MOST):
            slot = k * MOST + s
            turn[pl.ds(slot, H, stride=UNIT), :] = pieces[k][s * H : (s + 1) * H, :].astype(jnp.float32)
        first = H * UNIT + k * MOST
        turn[first : first + MOST, :] = pieces[k][MOST * H :, :].astype(jnp.float32)[:MOST]
    for a in range(FOLD):
        out[:, a * K : (a + 1) * K] = turn[a * UNIT : (a + 1) * UNIT, :].astype(out.dtype)


def unit_call(pieces):
    return pl.pallas_call(
        unit_kernel,
        out_shape=jax.ShapeDtypeStruct((UNIT, WIDTH), jnp.bfloat16),
        in_specs=[VMEM] * 8,
        out_specs=VMEM,
        scratch_shapes=[pltpu.VMEM((FOLD * UNIT, K), jnp.float32)],
        name="unit",
    )(*pieces)


def prepare_kernel(where, primal, dual, right, left, sems):
    at = pl.multiple_of((where[1] * 2 + where[2]) * K, K)
    copies = []
    for t in range(8):
        rows, here = pl.ds(t * K, K), pl.ds(at, K)
        copies.append((dual.at[rows, here], right.at[t, :, pl.ds(0, K)]))
        copies.append((primal.at[rows, here], right.at[t, :, pl.ds(K, K)]))
        copies.append((primal.at[here, rows], left.at[t, :, pl.ds(0, K)]))
        copies.append((dual.at[here, rows], left.at[t, :, pl.ds(K, K)]))
    started = [pltpu.make_async_copy(a, b, sems.at[n]) for n, (a, b) in enumerate(copies)]
    for c in started:
        c.start()
    for c in started:
        c.wait()


def prepare_call(where, primal, dual):
    return pl.pallas_call(
        prepare_kernel,
        out_shape=[jax.ShapeDtypeStruct((8, K, 2 * K), jnp.bfloat16)] * 2,
        in_specs=[SMEM, ANY, ANY],
        out_specs=[VMEM] * 2,
        scratch_shapes=[pltpu.SemaphoreType.DMA((32,))],
        name="prepare",
    )(where, primal, dual)


STRIDE = 40


def reduce_kernel(plan, chained, where, tiles, right, left, *refs):
    n = len(plan)
    blocks = refs[:n]
    rest = refs[n + (1 if chained else 0) :]
    out, held, turn, stage, sems = rest
    line, y, core = where[0], where[1], where[2]
    loads, spot = [], 0
    for b, (dy, dcore, first, size) in enumerate(plan):
        copy = pltpu.make_async_copy(blocks[b], held.at[pl.ds(spot, size)], sems.at[b])
        copy.start()
        loads.append((copy, spot))
        spot += size
    stores = []
    for b, (dy, dcore, first, size) in enumerate(plan):
        copy, spot = loads[b]
        row = lax.rem(y + dy, 4) * 64 + lax.rem(core + dcore, 2) * 32 + first
        copy.wait()
        for m in range(size):
            t = tiles[line * 256 + row + m]
            wide = jnp.dot(held[spot + m], right[t], preferred_element_type=jnp.float32)
            wide = wide.astype(jnp.bfloat16)
            tall = jnp.concatenate([wide[:, :K], wide[:, K:]], axis=0)
            both = jnp.dot(left[t], tall, preferred_element_type=jnp.float32)
            kept, last = folded(both, True)
            turn[pl.ds(m, H, stride=STRIDE), :] = kept
            turn[H * STRIDE + m : H * STRIDE + m + 1, :] = last
        for a in range(FOLD):
            rows = turn[a * STRIDE : a * STRIDE + size, :].astype(stage.dtype)
            stage[spot : spot + size, a * K : (a + 1) * K] = rows
        goal = out.at[pl.ds(pl.multiple_of(row, 16), size)]
        store = pltpu.make_async_copy(stage.at[pl.ds(spot, size)], goal, sems.at[n + b])
        store.start()
        stores.append(store)
    for store in stores:
        store.wait()


def reduce_call(plan, where, tiles, blocks, right, left, total):
    n = len(blocks)
    args = [where, tiles, right, left, *blocks]
    specs = [SMEM, SMEM, VMEM, VMEM] + [ANY] * n
    aliases = {}
    if total is not None:
        aliases = {len(args): 0}
        args.append(total)
        specs.append(ANY)
    return pl.pallas_call(
        functools.partial(reduce_kernel, plan, total is not None),
        out_shape=jax.ShapeDtypeStruct((256, WIDTH), jnp.bfloat16),
        in_specs=specs,
        out_specs=ANY,
        scratch_shapes=[
            pltpu.VMEM((64, K, K), jnp.bfloat16),
            pltpu.VMEM((FOLD * STRIDE, K), jnp.float32),
            pltpu.VMEM((64, WIDTH), jnp.bfloat16),
            pltpu.SemaphoreType.DMA((2 * n,)),
        ],
        input_output_aliases=aliases,
        name="reduced",
    )(*args)


def contract_kernel(n, *refs):
    units, total, outs = refs[:n], refs[n], refs[n + 1 :]
    rows = jnp.concatenate([u[...] for u in units], axis=0)
    values = lax.dot_general(rows, total[...], NT, preferred_element_type=jnp.float32)
    for m in range(n):
        outs[m][...] = values[m * UNIT : (m + 1) * UNIT]


def contract_call(units, total):
    n = len(units)
    return pl.pallas_call(
        functools.partial(contract_kernel, n),
        out_shape=[jax.ShapeDtypeStruct((UNIT, 256), jnp.float32)] * n,
        in_specs=[VMEM] * (n + 1),
        out_specs=[VMEM] * n,
        name="contract",
    )(*units, total)


def gather_kernel(known, late, where, *refs):
    n, m = len(known), len(late)
    values, units, total, out = refs[:n], refs[n : n + m], refs[n + m], refs[n + m + 1]
    x, z = where[0] // 4, lax.rem(where[0], 4)

    def group(d):
        return lax.rem(x - d[0] + 4, 4) * 4 + lax.rem(z - d[1] + 4, 4)

    for d, ref in zip(known, values):
        out[group(d)] = ref[...]
    rows = jnp.concatenate([u[...] for u in units], axis=0) if m > 1 else units[0][...]
    formed = lax.dot_general(rows, total[...], NT, preferred_element_type=jnp.float32)
    for k, d in enumerate(late):
        out[group(d)] = formed[k * UNIT : (k + 1) * UNIT]


def gather_call(where, known, late, total):
    return pl.pallas_call(
        functools.partial(gather_kernel, tuple(known), tuple(late)),
        out_shape=jax.ShapeDtypeStruct((16, UNIT, 256), jnp.float32),
        in_specs=[SMEM] + [VMEM] * (len(known) + len(late) + 1),
        out_specs=VMEM,
        name="gather",
    )(where, *known.values(), *late.values(), total)


def final_kernel(flags, places_ref, landed, out):
    for g in range(2):
        places = places_ref[:, g : g + 1]
        slots = lax.broadcasted_iota(jnp.int32, (256, 8 * UNIT), 1)
        hot = (slots == places).astype(jnp.bfloat16)
        values = jnp.concatenate([landed[c, g] for c in range(8)], axis=0)
        high = values.astype(jnp.bfloat16)
        rest = values - high.astype(jnp.float32)
        low = rest.astype(jnp.bfloat16)
        picked = jnp.dot(hot, high, preferred_element_type=jnp.float32)
        picked = picked + jnp.dot(hot, low, preferred_element_type=jnp.float32)
        turned = flags[g] > 0

        @pl.when(turned)
        def _():
            out[:, g * 256 : (g + 1) * 256] = picked

        @pl.when(jnp.logical_not(turned))
        def _():
            out[:, g * 256 : (g + 1) * 256] = picked.T


def final_call(flags, places, landed):
    return pl.pallas_call(
        final_kernel,
        out_shape=jax.ShapeDtypeStruct((256, 512), jnp.float32),
        in_specs=[SMEM, VMEM, VMEM],
        out_specs=VMEM,
        name="final",
    )(flags, places, landed)


def steps(coeffs, tiles, primal, dual_inverse):
    x, z = lax.axis_index("x"), lax.axis_index("z")
    y, core = lax.axis_index("y"), lax.axis_index("core")
    line = x * 4 + z
    tile = y * 2 + core
    where = jnp.stack([line, y, core]).astype(jnp.int32)
    flat = tiles.reshape(4096)

    pieces = fold_call(where, flat, coeffs)
    routed = [pieces[0]]
    for k in range(1, 8):
        routed.append(line_shift(pieces[k], k // 2, k % 2))
    units = {(0, 0): unit_call(routed)}
    right, left = prepare_call(where, primal, dual_inverse)

    other = line_shift(coeffs, 0, 1)
    down = line_shift(coeffs, 1, 0)
    up = line_shift(coeffs, 3, 0)
    down_other = line_shift(down, 0, 1)
    up_other = line_shift(up, 0, 1)
    low = line_shift(down[:16], 1, 0)
    high = line_shift(up[16:], 3, 0)
    low_other = line_shift(low, 0, 1)
    high_other = line_shift(high, 0, 1)

    def formed(plan, blocks, total):
        return reduce_call(plan, where, flat, blocks, right, left, total)

    total = formed(((0, 0, 0, 32), (0, 1, 0, 32)), [coeffs, other], None)
    total = formed(((3, 0, 0, 32), (3, 1, 0, 32)), [down, down_other], total)
    total = formed(((1, 0, 0, 32), (1, 1, 0, 32)), [up, up_other], total)
    plan = ((2, 0, 0, 16), (2, 0, 16, 16), (2, 1, 0, 16), (2, 1, 16, 16))
    total = formed(plan, [low, high, low_other, high_other], total)

    for d, parent in FIRST + SECOND + THIRD:
        shift = ((d[0] - parent[0]) % 4, (d[1] - parent[1]) % 4)
        units[d] = plane_shift(units[parent], shift)

    values = contract_call([units[d] for d in EARLY], total)
    known = dict(zip(EARLY, values))
    for d in EARLY:
        if negated(d) in TURNED:
            known[negated(d)] = plane_shift(known[d], negated(d))
    ordered = gather_call(where, known, {d: units[d] for d in LATE}, total)
    landed = lax.all_to_all(ordered.reshape(8, 2, UNIT, 256), LINE, 0, 0, tiled=True)

    ids = tiles.reshape(128, 32)
    earlier = jnp.tril(jnp.ones((32, 32), jnp.int32), -1)
    same = (ids[:, :, None] == ids[:, None, :]).astype(jnp.int32)
    ordinal = jnp.sum(same * earlier[None], axis=2)
    block = jnp.arange(128, dtype=jnp.int32)[:, None] % 8
    step = (ids // 2 - block // 2) % 4
    swapped = (ids + block) % 2
    place = ids * UNIT + step * 2 * MOST + swapped * MOST + ordinal
    place = place.reshape(16, 256)
    flips = np.array([0 if (a, b) in FORMED else 1 for a in range(4) for b in range(4)], np.int32)
    targets = tile * 2 + jnp.arange(2, dtype=jnp.int32)
    apart = (x - targets // 4) % 4 * 4 + (z - targets % 4) % 4
    flags = jnp.take(jnp.asarray(flips), apart)
    row_place = lax.dynamic_slice_in_dim(place, line, 1, 0)
    col_place = lax.dynamic_slice_in_dim(place, tile * 2, 2, 0)
    places = jnp.where(flags[:, None] > 0, row_place, col_place)
    return final_call(flags, places.T, landed)


def solution(mesh):
    finer = Mesh(mesh.devices.reshape(4, 4, 4, 2), ALL)
    in_specs = (P(ALL, None, None), P(), P(), P())
    out_specs = P(PLANE, LINE)
    return jax.shard_map(
        steps, mesh=finer, in_specs=in_specs, out_specs=out_specs, check_vma=False
    )
```

```python
import functools

import jax
import jax.numpy as jnp
from jax import lax
from jax.experimental import pallas as pl
from jax.experimental.pallas import tpu as pltpu
from jax.sharding import Mesh
from jax.sharding import PartitionSpec as P


MOST = 5
K = 128
H = 64
FOLD = H + 1
WIDTH = FOLD * K
UNIT = 8 * MOST
PIECE = MOST * H + 16
LINE = ("y", "core")
PLANE = ("x", "z")
ALL = ("x", "z", "y", "core")
NT = (((1,), (1,)), ((), ()))
VMEM = pl.BlockSpec(memory_space=pltpu.VMEM)
SMEM = pl.BlockSpec(memory_space=pltpu.SMEM)
HBM = pl.BlockSpec(memory_space=pltpu.HBM)

LIMIT = pltpu.CompilerParams(vmem_limit_bytes=20 << 20)


def near(x):
    return pltpu.with_memory_space_constraint(x, pltpu.VMEM)


def far(x):
    return pltpu.with_memory_space_constraint(x, pltpu.HBM)


def made(*shape, dtype=jnp.bfloat16):
    return pltpu.VMEM(shape, dtype)


FIRST = (((1, 0), (0, 0)), ((0, 3), (0, 0)), ((3, 1), (0, 0)))
SECOND = (((3, 3), (0, 3)), ((3, 2), (3, 1)), ((2, 3), (1, 0)))
THIRD = (((2, 0), (1, 0)), ((0, 2), (0, 3)), ((2, 2), (3, 2)))
EARLY = ((0, 0),) + tuple(d for d, _ in FIRST + SECOND)
LATE = tuple(d for d, _ in THIRD)
FORMED = EARLY + LATE


def negated(d):
    return ((-d[0]) % 4, (-d[1]) % 4)


TURNED = tuple(negated(d) for d in FORMED if negated(d) not in FORMED)


def plane_shift(x, shift):
    pairs = []
    for a in range(4):
        for b in range(4):
            pairs.append((a * 4 + b, (a + shift[0]) % 4 * 4 + (b + shift[1]) % 4))
    return lax.ppermute(x, PLANE, pairs)


def line_shift(x, shift, swap):
    pairs = []
    for a in range(4):
        for b in range(2):
            pairs.append((a * 2 + b, (a + shift) % 4 * 2 + (b + swap) % 2))
    return lax.ppermute(x, LINE, pairs)


def folded(square, half_diagonal):
    top, bottom = square[:H], square[H:]
    row = lax.broadcasted_iota(jnp.int32, (H, K), 0)
    lane = lax.broadcasted_iota(jnp.int32, (H, K), 1)
    turned = pltpu.roll(bottom, H, 1)
    kept = jnp.where(jnp.logical_and(lane < H, row > lane), turned, top)
    last = jnp.sum(jnp.where(lane == row + H, bottom, 0.0), axis=0, keepdims=True)
    if half_diagonal:
        kept = kept * jnp.where(row == lane, 0.5, 1.0)
        last = last * 0.5
    return kept, last


def fold_kernel(where, tiles, own_ref, *refs):
    outs, held, lasts, counts = refs[:8], refs[8], refs[9], refs[10]
    held[...] = jnp.zeros(held.shape, held.dtype)
    lasts[...] = jnp.zeros(lasts.shape, lasts.dtype)
    for k in range(8):
        counts[k] = 0
    y, core = where[1], where[2]
    mine = where[0] * 256 + y * 64 + core * 32

    def four(n, carry):
        for m in range(8):
            i = n * 8 + m
            t = tiles[mine + i]
            order = counts[t]
            counts[t] = order + 1
            goal = lax.rem(t // 2 - y + 4, 4) * 2 + lax.rem(t + core, 2)
            kept, last = folded(own_ref[i].astype(jnp.float32), False)
            row = pl.multiple_of(goal * PIECE + order * H, 16)
            held[pl.ds(row, H), :] = kept.astype(held.dtype)
            lasts[pl.ds(goal * 16 + order, 1), :] = last
        return carry

    lax.fori_loop(0, 4, four, 0)
    for k in range(8):
        outs[k][: MOST * H, :] = held[k * PIECE : k * PIECE + MOST * H, :]
        outs[k][MOST * H :, :] = lasts[k * 16 : (k + 1) * 16, :].astype(held.dtype)


def fold_call(where, tiles, own):
    return pl.pallas_call(
        fold_kernel,
        out_shape=[made(PIECE, K)] * 8,
        in_specs=[SMEM, SMEM, VMEM],
        out_specs=[VMEM] * 8,
        scratch_shapes=[
            pltpu.VMEM((8 * PIECE, K), jnp.bfloat16),
            pltpu.VMEM((8 * 16, K), jnp.float32),
            pltpu.SMEM((8,), jnp.int32),
        ],
        compiler_params=LIMIT,
        name="fold",
    )(where, tiles, own)


def unit_kernel(*refs):
    pieces, out, turn = refs[:8], refs[8], refs[9]
    for k in range(8):
        for s in range(MOST):
            slot = k * MOST + s
            turn[pl.ds(slot, H, stride=UNIT), :] = pieces[k][s * H : (s + 1) * H, :].astype(jnp.float32)
        first = H * UNIT + k * MOST
        turn[first : first + MOST, :] = pieces[k][MOST * H :, :].astype(jnp.float32)[:MOST]
    for a in range(FOLD):
        out[:, a * K : (a + 1) * K] = turn[a * UNIT : (a + 1) * UNIT, :].astype(out.dtype)


def unit_call(pieces):
    return pl.pallas_call(
        unit_kernel,
        out_shape=made(UNIT, WIDTH),
        in_specs=[VMEM] * 8,
        out_specs=VMEM,
        scratch_shapes=[pltpu.VMEM((FOLD * UNIT, K), jnp.float32)],
        compiler_params=LIMIT,
        name="unit",
    )(*[near(p) for p in pieces])


def prepare_kernel(where, primal, dual, right, left, sems):
    at = pl.multiple_of((where[1] * 2 + where[2]) * K, K)
    copies = []
    for t in range(8):
        rows, here = pl.ds(t * K, K), pl.ds(at, K)
        copies.append((dual.at[rows, here], right.at[t, :, pl.ds(0, K)]))
        copies.append((primal.at[rows, here], right.at[t, :, pl.ds(K, K)]))
        copies.append((primal.at[here, rows], left.at[t, :, pl.ds(0, K)]))
        copies.append((dual.at[here, rows], left.at[t, :, pl.ds(K, K)]))
    started = [pltpu.make_async_copy(a, b, sems.at[n]) for n, (a, b) in enumerate(copies)]
    for c in started:
        c.start()
    for c in started:
        c.wait()


def prepare_call(where, primal, dual):
    return pl.pallas_call(
        prepare_kernel,
        out_shape=[made(8, K, 2 * K)] * 2,
        in_specs=[SMEM, HBM, HBM],
        out_specs=[VMEM] * 2,
        scratch_shapes=[pltpu.SemaphoreType.DMA((32,))],
        compiler_params=LIMIT,
        name="prepare",
    )(where, far(primal), far(dual))


STRIDE = 40


def reduce_kernel(plan, chained, where, tiles, right, left, *refs):
    n = len(plan)
    blocks = refs[:n]
    out, *turns = refs[n + (1 if chained else 0) :]
    y, core = where[1], where[2]
    for b, (dy, dcore) in enumerate(plan):
        row = lax.rem(y + dy, 4) * 64 + lax.rem(core + dcore, 2) * 32
        turn = turns[b % 2]
        for m in range(32):
            t = tiles[row + m]
            wide = jnp.dot(blocks[b][m], right[t], preferred_element_type=jnp.float32)
            wide = wide.astype(jnp.bfloat16)
            tall = jnp.concatenate([wide[:, :K], wide[:, K:]], axis=0)
            both = jnp.dot(left[t], tall, preferred_element_type=jnp.float32)
            kept, last = folded(both, True)
            turn[pl.ds(m, H, stride=STRIDE), :] = kept
            turn[H * STRIDE + m : H * STRIDE + m + 1, :] = last
        rows = pl.ds(pl.multiple_of(row, 32), 32)
        for a in range(FOLD):
            part = turn[a * STRIDE : a * STRIDE + 32, :].astype(out.dtype)
            out[rows, a * K : (a + 1) * K] = part


def reduce_call(plan, where, tiles, blocks, right, left, total):
    n = len(blocks)
    args = [where, tiles, near(right), near(left), *[near(b) for b in blocks]]
    specs = [SMEM, SMEM, VMEM, VMEM] + [VMEM] * n
    aliases = {}
    if total is not None:
        aliases = {len(args): 0}
        args.append(near(total))
        specs.append(VMEM)
    return pl.pallas_call(
        functools.partial(reduce_kernel, plan, total is not None),
        out_shape=made(256, WIDTH),
        in_specs=specs,
        out_specs=VMEM,
        scratch_shapes=[
            pltpu.VMEM((FOLD * STRIDE, K), jnp.float32),
            pltpu.VMEM((FOLD * STRIDE, K), jnp.float32),
        ],
        input_output_aliases=aliases,
        compiler_params=LIMIT,
        name="reduced",
    )(*args)


def contract_kernel(n, *refs):
    units, total, outs = refs[:n], refs[n], refs[n + 1 :]
    rows = jnp.concatenate([u[...] for u in units], axis=0) if n > 1 else units[0][...]
    values = lax.dot_general(rows, total[...], NT, preferred_element_type=jnp.float32)
    for m in range(n):
        outs[m][...] = values[m * UNIT : (m + 1) * UNIT]


def contract_call(units, total):
    n = len(units)
    return pl.pallas_call(
        functools.partial(contract_kernel, n),
        out_shape=[made(UNIT, 256, dtype=jnp.float32)] * n,
        in_specs=[VMEM] * (n + 1),
        out_specs=[VMEM] * n,
        compiler_params=LIMIT,
        name="contract",
    )(*[near(u) for u in units], near(total))


def gather_kernel(known, where, *refs):
    values, out = refs[:-1], refs[-1]
    x, z = where[0] // 4, lax.rem(where[0], 4)
    for d, ref in zip(known, values):
        group = lax.rem(x - d[0] + 4, 4) * 4 + lax.rem(z - d[1] + 4, 4)
        out[group] = ref[...]


def gather_call(where, known):
    return pl.pallas_call(
        functools.partial(gather_kernel, tuple(known)),
        out_shape=made(16, UNIT, 256, dtype=jnp.float32),
        in_specs=[SMEM] + [VMEM] * len(known),
        out_specs=VMEM,
        compiler_params=LIMIT,
        name="gather",
    )(where, *[near(v) for v in known.values()])


FORMED_BITS = sum(1 << (d[0] * 4 + d[1]) for d in FORMED)


def final_kernel(where, ids_ref, landed, out):
    line, y, core = where[0], where[1], where[2]
    x, z = line // 4, lax.rem(line, 4)
    target = (y * 2 + core) * 2
    pairs = [ids_ref[pl.ds(2 * n, 2), :] for n in (line, target, target + 1)]
    ids = jnp.concatenate(pairs + [pairs[0]], axis=0)
    lane = lax.broadcasted_iota(jnp.int32, (8, K), 1)
    half = lax.broadcasted_iota(jnp.int32, (8, K), 0) % 2
    ordinal = jnp.zeros((8, K), jnp.int32)
    for s in range(1, 32):
        same = jnp.logical_and(pltpu.roll(ids, s, 1) == ids, (lane & 31) >= s)
        ordinal = ordinal + same.astype(jnp.int32)
    block = half * 4 + (lane >> 5)
    step = ((ids >> 1) - (block >> 1)) & 3
    place = ids * UNIT + step * (2 * MOST) + ((ids + block) & 1) * MOST + ordinal
    columns = place.T
    mine = jnp.concatenate([columns[:, 0:1], columns[:, 1:2]], axis=0)
    slots = lax.broadcasted_iota(jnp.int32, (256, 8 * UNIT), 1)
    for g in range(2):
        goal = target + g
        apart = lax.rem(x - goal // 4 + 4, 4) * 4 + lax.rem(z - lax.rem(goal, 4) + 4, 4)
        straight = (FORMED_BITS >> apart) & 1
        other = jnp.concatenate(
            [columns[:, 2 + 2 * g : 3 + 2 * g], columns[:, 3 + 2 * g : 4 + 2 * g]], axis=0
        )
        hot = (slots == jnp.where(straight > 0, other, mine)).astype(jnp.bfloat16)
        values = jnp.concatenate([landed[c, g] for c in range(8)], axis=0)
        high = values.astype(jnp.bfloat16)
        rest = values - high.astype(jnp.float32)
        low = rest.astype(jnp.bfloat16)
        picked = jnp.dot(hot, high, preferred_element_type=jnp.float32)
        picked = picked + jnp.dot(hot, low, preferred_element_type=jnp.float32)

        @pl.when(straight == 0)
        def _():
            out[:, g * 256 : (g + 1) * 256] = picked

        @pl.when(straight > 0)
        def _():
            out[:, g * 256 : (g + 1) * 256] = picked.T


def final_call(where, ids, landed):
    return pl.pallas_call(
        final_kernel,
        out_shape=jax.ShapeDtypeStruct((256, 512), jnp.float32),
        in_specs=[SMEM, VMEM, VMEM],
        out_specs=VMEM,
        compiler_params=LIMIT,
        name="final",
    )(where, ids, near(landed))


def steps(coeffs, tiles, primal, dual_inverse):
    x, z = lax.axis_index("x"), lax.axis_index("z")
    y, core = lax.axis_index("y"), lax.axis_index("core")
    line = x * 4 + z
    where = jnp.stack([line, y, core]).astype(jnp.int32)
    flat = tiles.reshape(4096)
    line_ids = lax.dynamic_slice_in_dim(flat, line * 256, 256, 0)

    pieces = fold_call(where, flat, coeffs)
    routed = [pieces[0]]
    for k in range(1, 8):
        routed.append(line_shift(pieces[k], k // 2, k % 2))
    units = {(0, 0): unit_call(routed)}
    right, left = prepare_call(where, primal, dual_inverse)

    other = line_shift(coeffs, 0, 1)
    down = line_shift(coeffs, 1, 0)
    up = line_shift(coeffs, 3, 0)
    across = line_shift(coeffs, 2, 0)
    down_other = line_shift(down, 0, 1)
    up_other = line_shift(up, 0, 1)
    across_other = line_shift(across, 0, 1)

    def formed(plan, blocks, total):
        return reduce_call(plan, where, line_ids, blocks, right, left, total)

    total = formed(((0, 0), (0, 1)), [coeffs, other], None)
    plan = ((3, 0), (3, 1), (1, 0), (1, 1))
    total = formed(plan, [down, down_other, up, up_other], total)
    total = formed(((2, 0), (2, 1)), [across, across_other], total)

    for d, parent in FIRST + SECOND + THIRD:
        shift = ((d[0] - parent[0]) % 4, (d[1] - parent[1]) % 4)
        units[d] = plane_shift(units[parent], shift)

    values = contract_call([units[d] for d in EARLY], total)
    known = dict(zip(EARLY, values))
    for d in EARLY:
        if negated(d) in TURNED:
            known[negated(d)] = plane_shift(known[d], negated(d))
    values = contract_call([units[d] for d in LATE], total)
    known.update(zip(LATE, values))
    ordered = gather_call(where, known)
    landed = lax.all_to_all(ordered.reshape(8, 2, UNIT, 256), LINE, 0, 0, tiled=True)

    return final_call(where, tiles.reshape(32, K), landed)


def solution(mesh):
    finer = Mesh(mesh.devices.reshape(4, 4, 4, 2), ALL)
    in_specs = (P(ALL, None, None), P(), P(), P())
    out_specs = P(PLANE, LINE)
    return jax.shard_map(
        steps, mesh=finer, in_specs=in_specs, out_specs=out_specs, check_vma=False
    )
```

```python
import functools

import jax
import jax.numpy as jnp
from jax import lax
from jax.experimental import pallas as pl
from jax.experimental.pallas import tpu as pltpu
from jax.sharding import Mesh
from jax.sharding import PartitionSpec as P


MOST = 5
K = 128
H = 64
FOLD = H + 1
WIDTH = FOLD * K
UNIT = 8 * MOST
PIECE = MOST * H + 16
LINE = ("y", "core")
PLANE = ("x", "z")
ALL = ("x", "z", "y", "core")
NT = (((1,), (1,)), ((), ()))
VMEM = pl.BlockSpec(memory_space=pltpu.VMEM)
SMEM = pl.BlockSpec(memory_space=pltpu.SMEM)
HBM = pl.BlockSpec(memory_space=pltpu.HBM)

LIMIT = pltpu.CompilerParams(vmem_limit_bytes=20 << 20)


def near(x):
    return pltpu.with_memory_space_constraint(x, pltpu.VMEM)


def far(x):
    return pltpu.with_memory_space_constraint(x, pltpu.HBM)


def made(*shape, dtype=jnp.bfloat16):
    return pltpu.VMEM(shape, dtype)


FIRST = (((1, 0), (0, 0)), ((0, 3), (0, 0)), ((3, 1), (0, 0)))
SECOND = (((3, 2), (3, 1)), ((2, 1), (3, 1)), ((2, 0), (1, 0)), ((0, 2), (0, 3)))
THIRD = (((1, 1), (1, 0)), ((2, 2), (3, 2)))
EARLY = ((0, 0),) + tuple(d for d, _ in FIRST + SECOND)
MIDDLE = ((1, 1),)
LATE = ((2, 2),)
FORMED = EARLY + MIDDLE + LATE


def negated(d):
    return ((-d[0]) % 4, (-d[1]) % 4)


TURNED = tuple(negated(d) for d in FORMED if negated(d) not in FORMED)


def plane_shift(x, shift):
    pairs = []
    for a in range(4):
        for b in range(4):
            pairs.append((a * 4 + b, (a + shift[0]) % 4 * 4 + (b + shift[1]) % 4))
    return lax.ppermute(x, PLANE, pairs)


def line_shift(x, shift, swap):
    pairs = []
    for a in range(4):
        for b in range(2):
            pairs.append((a * 2 + b, (a + shift) % 4 * 2 + (b + swap) % 2))
    return lax.ppermute(x, LINE, pairs)


def folded(square, half_diagonal):
    top, bottom = square[:H], square[H:]
    row = lax.broadcasted_iota(jnp.int32, (H, K), 0)
    lane = lax.broadcasted_iota(jnp.int32, (H, K), 1)
    turned = pltpu.roll(bottom, H, 1)
    kept = jnp.where(jnp.logical_and(lane < H, row > lane), turned, top)
    last = jnp.sum(jnp.where(lane == row + H, bottom, 0.0), axis=0, keepdims=True)
    if half_diagonal:
        kept = kept * jnp.where(row == lane, 0.5, 1.0)
        last = last * 0.5
    return kept, last


def unfolded(kept, last):
    row = lax.broadcasted_iota(jnp.int32, (H, K), 0)
    lane = lax.broadcasted_iota(jnp.int32, (H, K), 1)
    turned = kept.T
    wide = jnp.concatenate([turned, turned], axis=1)
    head, tail = wide[:H], wide[H:]
    top = jnp.where(jnp.logical_and(lane < H, row > lane), head, kept)
    corner = pltpu.roll(jnp.where(row > lane, kept, head), H, 1)
    right = jnp.where(lane == row + H, last, corner)
    return jnp.concatenate([top, jnp.where(lane < H, tail, right)], axis=0)


def fold_kernel(where, tiles, own_ref, *refs):
    outs, plain, held, lasts, ends, counts = refs[:8], *refs[8:]
    held[...] = jnp.zeros(held.shape, held.dtype)
    lasts[...] = jnp.zeros(lasts.shape, lasts.dtype)
    for k in range(8):
        counts[k] = 0
    y, core = where[1], where[2]
    mine = where[0] * 256 + y * 64 + core * 32

    def four(n, carry):
        for m in range(8):
            i = n * 8 + m
            t = tiles[mine + i]
            order = counts[t]
            counts[t] = order + 1
            goal = lax.rem(t // 2 - y + 4, 4) * 2 + lax.rem(t + core, 2)
            kept, last = folded(own_ref[i].astype(jnp.float32), False)
            row = pl.multiple_of(goal * PIECE + order * H, 16)
            kept = kept.astype(held.dtype)
            held[pl.ds(row, H), :] = kept
            plain[pl.ds(pl.multiple_of(i * H, H), H), :] = kept
            ends[pl.ds(i, 1), :] = last
            lasts[pl.ds(goal * 16 + order, 1), :] = last
        return carry

    lax.fori_loop(0, 4, four, 0)
    plain[32 * H :, :] = ends[...].astype(plain.dtype)
    for k in range(8):
        outs[k][: MOST * H, :] = held[k * PIECE : k * PIECE + MOST * H, :]
        outs[k][MOST * H :, :] = lasts[k * 16 : (k + 1) * 16, :].astype(held.dtype)


def fold_call(where, tiles, own):
    return pl.pallas_call(
        fold_kernel,
        out_shape=[made(PIECE, K)] * 8 + [made(32 * H + 32, K)],
        in_specs=[SMEM, SMEM, VMEM],
        out_specs=[VMEM] * 9,
        scratch_shapes=[
            pltpu.VMEM((8 * PIECE, K), jnp.bfloat16),
            pltpu.VMEM((8 * 16, K), jnp.float32),
            pltpu.VMEM((32, K), jnp.float32),
            pltpu.SMEM((8,), jnp.int32),
        ],
        compiler_params=LIMIT,
        name="fold",
    )(where, tiles, own)


def unit_kernel(*refs):
    pieces, out, turn = refs[:8], refs[8], refs[9]
    for k in range(8):
        for s in range(MOST):
            slot = k * MOST + s
            turn[pl.ds(slot, H, stride=UNIT), :] = pieces[k][s * H : (s + 1) * H, :].astype(jnp.float32)
        first = H * UNIT + k * MOST
        turn[first : first + MOST, :] = pieces[k][MOST * H :, :].astype(jnp.float32)[:MOST]
    for a in range(FOLD):
        out[:, a * K : (a + 1) * K] = turn[a * UNIT : (a + 1) * UNIT, :].astype(out.dtype)


def unit_call(pieces):
    return pl.pallas_call(
        unit_kernel,
        out_shape=made(UNIT, WIDTH),
        in_specs=[VMEM] * 8,
        out_specs=VMEM,
        scratch_shapes=[pltpu.VMEM((FOLD * UNIT, K), jnp.float32)],
        compiler_params=LIMIT,
        name="unit",
    )(*[near(p) for p in pieces])


def prepare_kernel(where, primal, dual, right, left, sems):
    at = pl.multiple_of((where[1] * 2 + where[2]) * K, K)
    copies = []
    for t in range(8):
        rows, here = pl.ds(t * K, K), pl.ds(at, K)
        copies.append((dual.at[rows, here], right.at[t, :, pl.ds(0, K)]))
        copies.append((primal.at[rows, here], right.at[t, :, pl.ds(K, K)]))
        copies.append((primal.at[here, rows], left.at[t, :, pl.ds(0, K)]))
        copies.append((dual.at[here, rows], left.at[t, :, pl.ds(K, K)]))
    started = [pltpu.make_async_copy(a, b, sems.at[n]) for n, (a, b) in enumerate(copies)]
    for c in started:
        c.start()
    for c in started:
        c.wait()


def prepare_call(where, primal, dual):
    return pl.pallas_call(
        prepare_kernel,
        out_shape=[made(8, K, 2 * K)] * 2,
        in_specs=[SMEM, HBM, HBM],
        out_specs=[VMEM] * 2,
        scratch_shapes=[pltpu.SemaphoreType.DMA((32,))],
        compiler_params=LIMIT,
        name="prepare",
    )(where, far(primal), far(dual))


STRIDE = 40


def reduce_kernel(plan, chained, where, tiles, right, left, *refs):
    n = len(plan)
    blocks = refs[:n]
    out, *turns = refs[n + (1 if chained else 0) :]
    y, core = where[1], where[2]
    for b, (dy, dcore) in enumerate(plan):
        row = lax.rem(y + dy, 4) * 64 + lax.rem(core + dcore, 2) * 32
        turn = turns[b % 2]
        packed = len(blocks[b].shape) == 2
        if packed:
            ends = blocks[b][32 * H :, :].astype(jnp.float32)
        for m in range(32):
            t = tiles[row + m]
            if packed:
                kept = blocks[b][m * H : (m + 1) * H, :].astype(jnp.float32)
                square = unfolded(kept, ends[m : m + 1]).astype(jnp.bfloat16)
            else:
                square = blocks[b][m]
            wide = jnp.dot(square, right[t], preferred_element_type=jnp.float32)
            wide = wide.astype(jnp.bfloat16)
            tall = jnp.concatenate([wide[:, :K], wide[:, K:]], axis=0)
            both = jnp.dot(left[t], tall, preferred_element_type=jnp.float32)
            kept, last = folded(both, True)
            turn[pl.ds(m, H, stride=STRIDE), :] = kept
            turn[H * STRIDE + m : H * STRIDE + m + 1, :] = last
        rows = pl.ds(pl.multiple_of(row, 32), 32)
        for a in range(FOLD):
            part = turn[a * STRIDE : a * STRIDE + 32, :].astype(out.dtype)
            out[rows, a * K : (a + 1) * K] = part


def reduce_call(plan, where, tiles, blocks, right, left, total):
    n = len(blocks)
    args = [where, tiles, near(right), near(left), *[near(b) for b in blocks]]
    specs = [SMEM, SMEM, VMEM, VMEM] + [VMEM] * n
    aliases = {}
    if total is not None:
        aliases = {len(args): 0}
        args.append(near(total))
        specs.append(VMEM)
    return pl.pallas_call(
        functools.partial(reduce_kernel, plan, total is not None),
        out_shape=made(256, WIDTH),
        in_specs=specs,
        out_specs=VMEM,
        scratch_shapes=[
            pltpu.VMEM((FOLD * STRIDE, K), jnp.float32),
            pltpu.VMEM((FOLD * STRIDE, K), jnp.float32),
        ],
        input_output_aliases=aliases,
        compiler_params=LIMIT,
        name="reduced",
    )(*args)


def contract_kernel(n, *refs):
    units, total, outs = refs[:n], refs[n], refs[n + 1 :]
    rows = jnp.concatenate([u[...] for u in units], axis=0) if n > 1 else units[0][...]
    values = lax.dot_general(rows, total[...], NT, preferred_element_type=jnp.float32)
    for m in range(n):
        outs[m][...] = values[m * UNIT : (m + 1) * UNIT]


def contract_call(units, total):
    n = len(units)
    return pl.pallas_call(
        functools.partial(contract_kernel, n),
        out_shape=[made(UNIT, 256, dtype=jnp.float32)] * n,
        in_specs=[VMEM] * (n + 1),
        out_specs=[VMEM] * n,
        compiler_params=LIMIT,
        name="contract",
    )(*[near(u) for u in units], near(total))


def gather_kernel(known, where, *refs):
    n = len(known)
    values, outs, held = refs[:n], refs[n : n + 8], refs[n + 8]
    x, z, y, core = where[0] // 4, lax.rem(where[0], 4), where[1], where[2]
    for d, ref in zip(known, values):
        column, row = lax.rem(x - d[0] + 4, 4), lax.rem(z - d[1] + 4, 4)
        goal = lax.rem(column - y + 4, 4) * 2 + lax.rem(row // 2 + core, 2)
        held[goal * 2 + lax.rem(row, 2)] = ref[...]
    for k in range(8):
        outs[k][...] = held[2 * k : 2 * k + 2]


def gather_call(where, known):
    return pl.pallas_call(
        functools.partial(gather_kernel, tuple(known)),
        out_shape=[made(2, UNIT, 256, dtype=jnp.float32)] * 8,
        in_specs=[SMEM] + [VMEM] * len(known),
        out_specs=[VMEM] * 8,
        scratch_shapes=[pltpu.VMEM((16, UNIT, 256), jnp.float32)],
        compiler_params=LIMIT,
        name="gather",
    )(where, *[near(v) for v in known.values()])


FORMED_BITS = sum(1 << (d[0] * 4 + d[1]) for d in FORMED)


def straight_of(where, g):
    x, z = where[0] // 4, lax.rem(where[0], 4)
    goal = (where[1] * 2 + where[2]) * 2 + g
    apart = lax.rem(x - goal // 4 + 4, 4) * 4 + lax.rem(z - lax.rem(goal, 4) + 4, 4)
    return goal, (FORMED_BITS >> apart) & 1


def places_kernel(where, ids_ref, hot_ref):
    line, y, core = where[0], where[1], where[2]
    goals = [straight_of(where, g) for g in range(2)]
    lines = [jnp.where(straight > 0, goal, line) for goal, straight in goals]
    pairs = [ids_ref[pl.ds(2 * n, 2), :] for n in lines]
    ids = jnp.concatenate(pairs + pairs, axis=0)
    lane = lax.broadcasted_iota(jnp.int32, (8, K), 1)
    half = lax.broadcasted_iota(jnp.int32, (8, K), 0) % 2
    ordinal = jnp.zeros((8, K), jnp.int32)
    for s in range(1, 32):
        same = jnp.logical_and(pltpu.roll(ids, s, 1) == ids, (lane & 31) >= s)
        ordinal = ordinal + same.astype(jnp.int32)
    block = half * 4 + (lane >> 5)
    step = ((ids >> 1) - (block >> 1)) & 3
    source = ((y - (ids >> 1)) & 3) * 2 + ((ids + core) & 1)
    place = source * UNIT + step * (2 * MOST) + ((ids + block) & 1) * MOST + ordinal
    columns = place.T
    slots = lax.broadcasted_iota(jnp.int32, (256, 8 * UNIT), 1)
    for g in range(2):
        chosen = jnp.concatenate(
            [columns[:, 2 * g : 2 * g + 1], columns[:, 2 * g + 1 : 2 * g + 2]], axis=0
        )
        hot_ref[g] = (slots == chosen).astype(hot_ref.dtype)


def places_call(where, ids):
    return pl.pallas_call(
        places_kernel,
        out_shape=made(2, 256, 8 * UNIT),
        in_specs=[SMEM, VMEM],
        out_specs=VMEM,
        compiler_params=LIMIT,
        name="places",
    )(where, ids)


def final_kernel(where, hot_ref, *refs):
    landed, out = refs[:8], refs[8]
    for g in range(2):
        _, straight = straight_of(where, g)
        values = jnp.concatenate([ref[g] for ref in landed], axis=0)
        high = values.astype(jnp.bfloat16)
        low = (values - high.astype(jnp.float32)).astype(jnp.bfloat16)
        hot = hot_ref[g]
        picked = jnp.dot(hot, high, preferred_element_type=jnp.float32)
        picked = picked + jnp.dot(hot, low, preferred_element_type=jnp.float32)

        @pl.when(straight == 0)
        def _():
            out[:, g * 256 : (g + 1) * 256] = picked

        @pl.when(straight > 0)
        def _():
            out[:, g * 256 : (g + 1) * 256] = picked.T


def final_call(where, hot, landed):
    return pl.pallas_call(
        final_kernel,
        out_shape=jax.ShapeDtypeStruct((256, 512), jnp.float32),
        in_specs=[SMEM] + [VMEM] * 9,
        out_specs=VMEM,
        compiler_params=LIMIT,
        name="final",
    )(where, near(hot), *[near(v) for v in landed])


def steps(coeffs, tiles, primal, dual_inverse):
    x, z = lax.axis_index("x"), lax.axis_index("z")
    y, core = lax.axis_index("y"), lax.axis_index("core")
    line = x * 4 + z
    where = jnp.stack([line, y, core]).astype(jnp.int32)
    flat = tiles.reshape(4096)
    line_ids = lax.dynamic_slice_in_dim(flat, line * 256, 256, 0)

    *pieces, plain = fold_call(where, flat, coeffs)
    routed = [pieces[0]]
    for k in range(1, 8):
        routed.append(line_shift(pieces[k], k // 2, k % 2))
    units = {(0, 0): unit_call(routed)}
    right, left = prepare_call(where, primal, dual_inverse)

    other = line_shift(coeffs, 0, 1)
    down = line_shift(plain, 1, 0)
    up = line_shift(plain, 3, 0)
    across = line_shift(plain, 2, 0)
    down_other = line_shift(down, 0, 1)
    up_other = line_shift(up, 0, 1)
    across_other = line_shift(across, 0, 1)

    def formed(plan, blocks, total):
        return reduce_call(plan, where, line_ids, blocks, right, left, total)

    total = formed(((0, 0), (0, 1)), [coeffs, other], None)
    total = formed(((3, 0), (3, 1)), [down, down_other], total)
    total = formed(((1, 0), (1, 1)), [up, up_other], total)
    total = formed(((2, 0), (2, 1)), [across, across_other], total)

    for d, parent in FIRST + SECOND + THIRD:
        shift = ((d[0] - parent[0]) % 4, (d[1] - parent[1]) % 4)
        units[d] = plane_shift(units[parent], shift)

    known = {}
    for part in (EARLY, MIDDLE, LATE):
        values = contract_call([units[d] for d in part], total)
        known.update(zip(part, values))
    for d in EARLY + MIDDLE:
        if negated(d) in TURNED:
            known[negated(d)] = plane_shift(known[d], negated(d))
    ordered = gather_call(where, known)
    landed = [ordered[0]]
    for k in range(1, 8):
        landed.append(line_shift(ordered[k], k // 2, k % 2))
    hot = places_call(where, tiles.reshape(32, K))
    return final_call(where, hot, landed)


def solution(mesh):
    finer = Mesh(mesh.devices.reshape(4, 4, 4, 2), ALL)
    in_specs = (P(ALL, None, None), P(), P(), P())
    out_specs = P(PLANE, LINE)
    return jax.shard_map(
        steps, mesh=finer, in_specs=in_specs, out_specs=out_specs, check_vma=False
    )
```

```python
import functools

import jax
import jax.numpy as jnp
from jax import lax
from jax.experimental import pallas as pl
from jax.experimental.pallas import tpu as pltpu
from jax.sharding import Mesh
from jax.sharding import PartitionSpec as P


MOST = 5
K = 128
H = 64
FOLD = H + 1
WIDTH = FOLD * K
UNIT = 8 * MOST
PIECE = MOST * H + 16
LINE = ("y", "core")
PLANE = ("x", "z")
ALL = ("x", "z", "y", "core")
NT = (((1,), (1,)), ((), ()))
VMEM = pl.BlockSpec(memory_space=pltpu.VMEM)
SMEM = pl.BlockSpec(memory_space=pltpu.SMEM)
HBM = pl.BlockSpec(memory_space=pltpu.HBM)

LIMIT = pltpu.CompilerParams(vmem_limit_bytes=20 << 20)


def near(x):
    return pltpu.with_memory_space_constraint(x, pltpu.VMEM)


def far(x):
    return pltpu.with_memory_space_constraint(x, pltpu.HBM)


def made(*shape, dtype=jnp.bfloat16):
    return pltpu.VMEM(shape, dtype)


FIRST = (((1, 0), (0, 0)), ((0, 3), (0, 0)), ((3, 1), (0, 0)))
SECOND = (((3, 2), (3, 1)), ((2, 1), (3, 1)), ((2, 0), (1, 0)), ((0, 2), (0, 3)))
THIRD = (((1, 1), (1, 0)), ((2, 2), (3, 2)))
EARLY = ((0, 0),) + tuple(d for d, _ in FIRST + SECOND)
MIDDLE = ((1, 1),)
LATE = ((2, 2),)
FORMED = EARLY + MIDDLE + LATE


def negated(d):
    return ((-d[0]) % 4, (-d[1]) % 4)


TURNED = tuple(negated(d) for d in FORMED if negated(d) not in FORMED)


def plane_shift(x, shift):
    pairs = []
    for a in range(4):
        for b in range(4):
            pairs.append((a * 4 + b, (a + shift[0]) % 4 * 4 + (b + shift[1]) % 4))
    return lax.ppermute(x, PLANE, pairs)


def line_shift(x, shift, swap):
    pairs = []
    for a in range(4):
        for b in range(2):
            pairs.append((a * 2 + b, (a + shift) % 4 * 2 + (b + swap) % 2))
    return lax.ppermute(x, LINE, pairs)


def folded(square, half_diagonal):
    top, bottom = square[:H], square[H:]
    row = lax.broadcasted_iota(jnp.int32, (H, K), 0)
    lane = lax.broadcasted_iota(jnp.int32, (H, K), 1)
    turned = pltpu.roll(bottom, H, 1)
    kept = jnp.where(jnp.logical_and(lane < H, row > lane), turned, top)
    last = jnp.sum(jnp.where(lane == row + H, bottom, 0.0), axis=0, keepdims=True)
    if half_diagonal:
        kept = kept * jnp.where(row == lane, 0.5, 1.0)
        last = last * 0.5
    return kept, last


def unfolded(kept, last):
    row = lax.broadcasted_iota(jnp.int32, (H, K), 0)
    lane = lax.broadcasted_iota(jnp.int32, (H, K), 1)
    wide = jnp.concatenate([kept, kept], axis=0).T
    head, tail = wide[:H], wide[H:]
    top = jnp.where(jnp.logical_and(lane < H, row > lane), head, kept)
    corner = pltpu.roll(jnp.where(row > lane, kept, head), H, 1)
    right = jnp.where(lane == row + H, last, corner)
    return jnp.concatenate([top, jnp.where(lane < H, tail, right)], axis=0)


def fold_kernel(where, tiles, own_ref, *refs):
    outs, plain, held, lasts, ends, counts = refs[:8], *refs[8:]
    held[...] = jnp.zeros(held.shape, held.dtype)
    lasts[...] = jnp.zeros(lasts.shape, lasts.dtype)
    for k in range(8):
        counts[k] = 0
    y, core = where[1], where[2]
    mine = where[0] * 256 + y * 64 + core * 32

    def four(n, carry):
        for m in range(8):
            i = n * 8 + m
            t = tiles[mine + i]
            order = counts[t]
            counts[t] = order + 1
            goal = lax.rem(t // 2 - y + 4, 4) * 2 + lax.rem(t + core, 2)
            kept, last = folded(own_ref[i].astype(jnp.float32), False)
            row = pl.multiple_of(goal * PIECE + order * H, 16)
            kept = kept.astype(held.dtype)
            held[pl.ds(row, H), :] = kept
            plain[pl.ds(pl.multiple_of(i * H, H), H), :] = kept
            ends[pl.ds(i, 1), :] = last
            lasts[pl.ds(goal * 16 + order, 1), :] = last
        return carry

    lax.fori_loop(0, 4, four, 0)
    plain[32 * H :, :] = ends[...].astype(plain.dtype)
    for k in range(8):
        outs[k][: MOST * H, :] = held[k * PIECE : k * PIECE + MOST * H, :]
        outs[k][MOST * H :, :] = lasts[k * 16 : (k + 1) * 16, :].astype(held.dtype)


def fold_call(where, tiles, own):
    return pl.pallas_call(
        fold_kernel,
        out_shape=[made(PIECE, K)] * 8 + [made(32 * H + 32, K)],
        in_specs=[SMEM, SMEM, VMEM],
        out_specs=[VMEM] * 9,
        scratch_shapes=[
            pltpu.VMEM((8 * PIECE, K), jnp.bfloat16),
            pltpu.VMEM((8 * 16, K), jnp.float32),
            pltpu.VMEM((32, K), jnp.float32),
            pltpu.SMEM((8,), jnp.int32),
        ],
        compiler_params=LIMIT,
        name="fold",
    )(where, tiles, own)


def unit_kernel(*refs):
    pieces, out, turn = refs[:8], refs[8], refs[9]
    for k in range(8):
        for s in range(MOST):
            slot = k * MOST + s
            turn[pl.ds(slot, H, stride=UNIT), :] = pieces[k][s * H : (s + 1) * H, :].astype(jnp.float32)
        first = H * UNIT + k * MOST
        turn[first : first + MOST, :] = pieces[k][MOST * H :, :].astype(jnp.float32)[:MOST]
    for a in range(FOLD):
        out[:, a * K : (a + 1) * K] = turn[a * UNIT : (a + 1) * UNIT, :].astype(out.dtype)


def unit_call(pieces):
    return pl.pallas_call(
        unit_kernel,
        out_shape=made(UNIT, WIDTH),
        in_specs=[VMEM] * 8,
        out_specs=VMEM,
        scratch_shapes=[pltpu.VMEM((FOLD * UNIT, K), jnp.float32)],
        compiler_params=LIMIT,
        name="unit",
    )(*[near(p) for p in pieces])


def prepare_kernel(where, primal, dual, right, left, sems):
    at = pl.multiple_of((where[1] * 2 + where[2]) * K, K)
    copies = []
    for t in range(8):
        rows, here = pl.ds(t * K, K), pl.ds(at, K)
        copies.append((dual.at[rows, here], right.at[t, :, pl.ds(0, K)]))
        copies.append((primal.at[rows, here], right.at[t, :, pl.ds(K, K)]))
        copies.append((primal.at[here, rows], left.at[t, :, pl.ds(0, K)]))
        copies.append((dual.at[here, rows], left.at[t, :, pl.ds(K, K)]))
    started = [pltpu.make_async_copy(a, b, sems.at[n]) for n, (a, b) in enumerate(copies)]
    for c in started:
        c.start()
    for c in started:
        c.wait()


def prepare_call(where, primal, dual):
    return pl.pallas_call(
        prepare_kernel,
        out_shape=[made(8, K, 2 * K)] * 2,
        in_specs=[SMEM, HBM, HBM],
        out_specs=[VMEM] * 2,
        scratch_shapes=[pltpu.SemaphoreType.DMA((32,))],
        compiler_params=LIMIT,
        name="prepare",
    )(where, far(primal), far(dual))


STRIDE = 40


def reduce_kernel(plan, chained, where, tiles, right, left, *refs):
    n = len(plan)
    blocks = refs[:n]
    out, *turns = refs[n + (1 if chained else 0) :]
    y, core = where[1], where[2]
    for b, (dy, dcore) in enumerate(plan):
        row = lax.rem(y + dy, 4) * 64 + lax.rem(core + dcore, 2) * 32
        turn = turns[b % 2]
        packed = len(blocks[b].shape) == 2
        if packed:
            ends = blocks[b][32 * H :, :].astype(jnp.float32)
        for m in range(32):
            t = tiles[row + m]
            if packed:
                kept = blocks[b][m * H : (m + 1) * H, :].astype(jnp.float32)
                square = unfolded(kept, ends[m : m + 1]).astype(jnp.bfloat16)
            else:
                square = blocks[b][m]
            wide = jnp.dot(square, right[t], preferred_element_type=jnp.float32)
            wide = wide.astype(jnp.bfloat16)
            tall = jnp.concatenate([wide[:, :K], wide[:, K:]], axis=0)
            both = jnp.dot(left[t], tall, preferred_element_type=jnp.float32)
            kept, last = folded(both, True)
            turn[pl.ds(m, H, stride=STRIDE), :] = kept
            turn[H * STRIDE + m : H * STRIDE + m + 1, :] = last
        rows = pl.ds(pl.multiple_of(row, 32), 32)
        for a in range(FOLD):
            part = turn[a * STRIDE : a * STRIDE + 32, :].astype(out.dtype)
            out[rows, a * K : (a + 1) * K] = part


def reduce_call(plan, where, tiles, blocks, right, left, total):
    n = len(blocks)
    args = [where, tiles, near(right), near(left), *[near(b) for b in blocks]]
    specs = [SMEM, SMEM, VMEM, VMEM] + [VMEM] * n
    aliases = {}
    if total is not None:
        aliases = {len(args): 0}
        args.append(near(total))
        specs.append(VMEM)
    return pl.pallas_call(
        functools.partial(reduce_kernel, plan, total is not None),
        out_shape=made(256, WIDTH),
        in_specs=specs,
        out_specs=VMEM,
        scratch_shapes=[
            pltpu.VMEM((FOLD * STRIDE, K), jnp.float32),
            pltpu.VMEM((FOLD * STRIDE, K), jnp.float32),
        ],
        input_output_aliases=aliases,
        compiler_params=LIMIT,
        name="reduced",
    )(*args)


def contract_kernel(n, *refs):
    units, total, outs = refs[:n], refs[n], refs[n + 1 :]
    rows = jnp.concatenate([u[...] for u in units], axis=0) if n > 1 else units[0][...]
    values = lax.dot_general(rows, total[...], NT, preferred_element_type=jnp.float32)
    for m in range(n):
        outs[m][...] = values[m * UNIT : (m + 1) * UNIT]


def contract_call(units, total):
    n = len(units)
    return pl.pallas_call(
        functools.partial(contract_kernel, n),
        out_shape=[made(UNIT, 256, dtype=jnp.float32)] * n,
        in_specs=[VMEM] * (n + 1),
        out_specs=[VMEM] * n,
        compiler_params=LIMIT,
        name="contract",
    )(*[near(u) for u in units], near(total))


def gather_kernel(known, where, *refs):
    n = len(known)
    values, outs, held = refs[:n], refs[n : n + 8], refs[n + 8]
    x, z, y, core = where[0] // 4, lax.rem(where[0], 4), where[1], where[2]
    for d, ref in zip(known, values):
        column, row = lax.rem(x - d[0] + 4, 4), lax.rem(z - d[1] + 4, 4)
        goal = lax.rem(column - y + 4, 4) * 2 + lax.rem(row // 2 + core, 2)
        held[goal * 2 + lax.rem(row, 2)] = ref[...]
    for k in range(8):
        outs[k][...] = held[2 * k : 2 * k + 2]


def gather_call(where, known):
    return pl.pallas_call(
        functools.partial(gather_kernel, tuple(known)),
        out_shape=[made(2, UNIT, 256, dtype=jnp.float32)] * 8,
        in_specs=[SMEM] + [VMEM] * len(known),
        out_specs=[VMEM] * 8,
        scratch_shapes=[pltpu.VMEM((16, UNIT, 256), jnp.float32)],
        compiler_params=LIMIT,
        name="gather",
    )(where, *[near(v) for v in known.values()])


FORMED_BITS = sum(1 << (d[0] * 4 + d[1]) for d in FORMED)


def straight_of(where, g):
    x, z = where[0] // 4, lax.rem(where[0], 4)
    goal = (where[1] * 2 + where[2]) * 2 + g
    apart = lax.rem(x - goal // 4 + 4, 4) * 4 + lax.rem(z - lax.rem(goal, 4) + 4, 4)
    return goal, (FORMED_BITS >> apart) & 1


def places_kernel(where, ids_ref, hot_ref):
    line, y, core = where[0], where[1], where[2]
    goals = [straight_of(where, g) for g in range(2)]
    lines = [jnp.where(straight > 0, goal, line) for goal, straight in goals]
    pairs = [ids_ref[pl.ds(2 * n, 2), :] for n in lines]
    ids = jnp.concatenate(pairs + pairs, axis=0)
    lane = lax.broadcasted_iota(jnp.int32, (8, K), 1)
    half = lax.broadcasted_iota(jnp.int32, (8, K), 0) % 2
    ordinal = jnp.zeros((8, K), jnp.int32)
    for s in range(1, 32):
        same = jnp.logical_and(pltpu.roll(ids, s, 1) == ids, (lane & 31) >= s)
        ordinal = ordinal + same.astype(jnp.int32)
    block = half * 4 + (lane >> 5)
    step = ((ids >> 1) - (block >> 1)) & 3
    source = ((y - (ids >> 1)) & 3) * 2 + ((ids + core) & 1)
    place = source * UNIT + step * (2 * MOST) + ((ids + block) & 1) * MOST + ordinal
    columns = place.T
    slots = lax.broadcasted_iota(jnp.int32, (256, 8 * UNIT), 1)
    for g in range(2):
        chosen = jnp.concatenate(
            [columns[:, 2 * g : 2 * g + 1], columns[:, 2 * g + 1 : 2 * g + 2]], axis=0
        )
        hot_ref[g] = (slots == chosen).astype(hot_ref.dtype)


def places_call(where, ids):
    return pl.pallas_call(
        places_kernel,
        out_shape=made(2, 256, 8 * UNIT),
        in_specs=[SMEM, VMEM],
        out_specs=VMEM,
        compiler_params=LIMIT,
        name="places",
    )(where, ids)


def final_kernel(where, hot_ref, *refs):
    landed, out, held, sems = refs[:8], *refs[8:]
    stores = []
    for g in range(2):
        _, straight = straight_of(where, g)
        values = jnp.concatenate([ref[g] for ref in landed], axis=0)
        high = values.astype(jnp.bfloat16)
        low = (values - high.astype(jnp.float32)).astype(jnp.bfloat16)
        hot = hot_ref[g]
        picked = jnp.dot(hot, high, preferred_element_type=jnp.float32)
        picked = picked + jnp.dot(hot, low, preferred_element_type=jnp.float32)

        @pl.when(straight == 0)
        def _():
            held[g] = picked

        @pl.when(straight > 0)
        def _():
            held[g] = picked.T

        store = pltpu.make_async_copy(held.at[g], out.at[:, pl.ds(g * 256, 256)], sems.at[g])
        store.start()
        stores.append(store)
    for store in stores:
        store.wait()


def final_call(where, hot, landed):
    return pl.pallas_call(
        final_kernel,
        out_shape=jax.ShapeDtypeStruct((256, 512), jnp.float32),
        in_specs=[SMEM] + [VMEM] * 9,
        out_specs=HBM,
        scratch_shapes=[
            pltpu.VMEM((2, 256, 256), jnp.float32),
            pltpu.SemaphoreType.DMA((2,)),
        ],
        compiler_params=LIMIT,
        name="final",
    )(where, near(hot), *[near(v) for v in landed])


def steps(coeffs, tiles, primal, dual_inverse):
    x, z = lax.axis_index("x"), lax.axis_index("z")
    y, core = lax.axis_index("y"), lax.axis_index("core")
    line = x * 4 + z
    where = jnp.stack([line, y, core]).astype(jnp.int32)
    flat = tiles.reshape(4096)
    line_ids = lax.dynamic_slice_in_dim(flat, line * 256, 256, 0)

    *pieces, plain = fold_call(where, flat, coeffs)
    routed = [pieces[0]]
    for k in range(1, 8):
        routed.append(line_shift(pieces[k], k // 2, k % 2))
    units = {(0, 0): unit_call(routed)}
    right, left = prepare_call(where, primal, dual_inverse)

    other = line_shift(coeffs, 0, 1)
    down = line_shift(plain, 1, 0)
    up = line_shift(plain, 3, 0)
    across = line_shift(plain, 2, 0)
    down_other = line_shift(down, 0, 1)
    up_other = line_shift(up, 0, 1)
    across_other = line_shift(across, 0, 1)

    def formed(plan, blocks, total):
        return reduce_call(plan, where, line_ids, blocks, right, left, total)

    total = formed(((0, 0), (0, 1)), [coeffs, other], None)
    total = formed(((3, 0), (3, 1)), [down, down_other], total)
    total = formed(((1, 0), (1, 1)), [up, up_other], total)
    total = formed(((2, 0), (2, 1)), [across, across_other], total)

    for d, parent in FIRST + SECOND + THIRD:
        shift = ((d[0] - parent[0]) % 4, (d[1] - parent[1]) % 4)
        units[d] = plane_shift(units[parent], shift)

    known = {}
    for part in (EARLY, MIDDLE, LATE):
        values = contract_call([units[d] for d in part], total)
        known.update(zip(part, values))
    for d in EARLY + MIDDLE:
        if negated(d) in TURNED:
            known[negated(d)] = plane_shift(known[d], negated(d))
    ordered = gather_call(where, known)
    landed = [ordered[0]]
    for k in range(1, 8):
        landed.append(line_shift(ordered[k], k // 2, k % 2))
    hot = places_call(where, tiles.reshape(32, K))
    return final_call(where, hot, landed)


def solution(mesh):
    finer = Mesh(mesh.devices.reshape(4, 4, 4, 2), ALL)
    in_specs = (P(ALL, None, None), P(), P(), P())
    out_specs = P(PLANE, LINE)
    return jax.shard_map(
        steps, mesh=finer, in_specs=in_specs, out_specs=out_specs, check_vma=False
    )
```

```python
import functools

import jax
import jax.numpy as jnp
from jax import lax
from jax.experimental import pallas as pl
from jax.experimental.pallas import tpu as pltpu
from jax.sharding import Mesh
from jax.sharding import PartitionSpec as P


MOST = 5
K = 128
H = 64
FOLD = H + 1
WIDTH = FOLD * K
UNIT = 8 * MOST
PIECE = MOST * H + 16
LINE = ("y", "core")
PLANE = ("x", "z")
ALL = ("x", "z", "y", "core")
NT = (((1,), (1,)), ((), ()))
VMEM = pl.BlockSpec(memory_space=pltpu.VMEM)
SMEM = pl.BlockSpec(memory_space=pltpu.SMEM)
HBM = pl.BlockSpec(memory_space=pltpu.HBM)

LIMIT = pltpu.CompilerParams(vmem_limit_bytes=20 << 20)


def near(x):
    return pltpu.with_memory_space_constraint(x, pltpu.VMEM)


def far(x):
    return pltpu.with_memory_space_constraint(x, pltpu.HBM)


def made(*shape, dtype=jnp.bfloat16):
    return pltpu.VMEM(shape, dtype)


FIRST = (((1, 0), (0, 0)), ((0, 3), (0, 0)), ((3, 1), (0, 0)))
SECOND = (((3, 2), (3, 1)), ((2, 1), (3, 1)), ((2, 0), (1, 0)), ((0, 2), (0, 3)))
THIRD = (((1, 1), (1, 0)), ((2, 2), (3, 2)))
EARLY = ((0, 0),) + tuple(d for d, _ in FIRST + SECOND)
MIDDLE = ((1, 1),)
LATE = ((2, 2),)
FORMED = EARLY + MIDDLE + LATE


def negated(d):
    return ((-d[0]) % 4, (-d[1]) % 4)


TURNED = tuple(negated(d) for d in FORMED if negated(d) not in FORMED)


def plane_shift(x, shift):
    pairs = []
    for a in range(4):
        for b in range(4):
            pairs.append((a * 4 + b, (a + shift[0]) % 4 * 4 + (b + shift[1]) % 4))
    return lax.ppermute(x, PLANE, pairs)


def line_shift(x, shift, swap):
    pairs = []
    for a in range(4):
        for b in range(2):
            pairs.append((a * 2 + b, (a + shift) % 4 * 2 + (b + swap) % 2))
    return lax.ppermute(x, LINE, pairs)


def folded(square, half_diagonal):
    top, bottom = square[:H], square[H:]
    row = lax.broadcasted_iota(jnp.int32, (H, K), 0)
    lane = lax.broadcasted_iota(jnp.int32, (H, K), 1)
    turned = pltpu.roll(bottom, H, 1)
    kept = jnp.where(jnp.logical_and(lane < H, row > lane), turned, top)
    last = jnp.sum(jnp.where(lane == row + H, bottom, 0.0), axis=0, keepdims=True)
    if half_diagonal:
        kept = kept * jnp.where(row == lane, 0.5, 1.0)
        last = last * 0.5
    return kept, last


def unfolded(kept, last):
    row = lax.broadcasted_iota(jnp.int32, (H, K), 0)
    lane = lax.broadcasted_iota(jnp.int32, (H, K), 1)
    wide = jnp.concatenate([kept, kept], axis=0).T
    head, tail = wide[:H], wide[H:]
    top = jnp.where(jnp.logical_and(lane < H, row > lane), head, kept)
    corner = pltpu.roll(jnp.where(row > lane, kept, head), H, 1)
    right = jnp.where(lane == row + H, last, corner)
    return jnp.concatenate([top, jnp.where(lane < H, tail, right)], axis=0)


def fold_kernel(where, tiles, own_ref, *refs):
    outs, plain, held, lasts, ends, counts, near_ref, sems = refs[:8], *refs[8:]
    loads = []
    for n in range(4):
        rows = pl.ds(n * 8, 8)
        loads.append(pltpu.make_async_copy(own_ref.at[rows], near_ref.at[rows], sems.at[n]))
        loads[n].start()
    held[...] = jnp.zeros(held.shape, held.dtype)
    lasts[...] = jnp.zeros(lasts.shape, lasts.dtype)
    for k in range(8):
        counts[k] = 0
    y, core = where[1], where[2]
    mine = where[0] * 256 + y * 64 + core * 32

    for n in range(4):
        loads[n].wait()
        for m in range(8):
            i = n * 8 + m
            t = tiles[mine + i]
            order = counts[t]
            counts[t] = order + 1
            goal = lax.rem(t // 2 - y + 4, 4) * 2 + lax.rem(t + core, 2)
            kept, last = folded(near_ref[i].astype(jnp.float32), False)
            row = pl.multiple_of(goal * PIECE + order * H, 16)
            kept = kept.astype(held.dtype)
            held[pl.ds(row, H), :] = kept
            plain[i * H : (i + 1) * H, :] = kept
            ends[i : i + 1, :] = last
            lasts[pl.ds(goal * 16 + order, 1), :] = last
    plain[32 * H :, :] = ends[...].astype(plain.dtype)
    for k in range(8):
        outs[k][: MOST * H, :] = held[k * PIECE : k * PIECE + MOST * H, :]
        outs[k][MOST * H :, :] = lasts[k * 16 : (k + 1) * 16, :].astype(held.dtype)


def fold_call(where, tiles, own):
    return pl.pallas_call(
        fold_kernel,
        out_shape=[made(PIECE, K)] * 8 + [made(32 * H + 32, K)],
        in_specs=[SMEM, SMEM, HBM],
        out_specs=[VMEM] * 9,
        scratch_shapes=[
            pltpu.VMEM((8 * PIECE, K), jnp.bfloat16),
            pltpu.VMEM((8 * 16, K), jnp.float32),
            pltpu.VMEM((32, K), jnp.float32),
            pltpu.SMEM((8,), jnp.int32),
            pltpu.VMEM((32, K, K), jnp.bfloat16),
            pltpu.SemaphoreType.DMA((4,)),
        ],
        compiler_params=LIMIT,
        name="fold",
    )(where, far(tiles), far(own))


def unit_kernel(*refs):
    pieces, out, turn = refs[:8], refs[8], refs[9]
    for k in range(8):
        for s in range(MOST):
            slot = k * MOST + s
            turn[pl.ds(slot, H, stride=UNIT), :] = pieces[k][s * H : (s + 1) * H, :].astype(jnp.float32)
        first = H * UNIT + k * MOST
        turn[first : first + MOST, :] = pieces[k][MOST * H :, :].astype(jnp.float32)[:MOST]
    for a in range(FOLD):
        out[:, a * K : (a + 1) * K] = turn[a * UNIT : (a + 1) * UNIT, :].astype(out.dtype)


def unit_call(pieces):
    return pl.pallas_call(
        unit_kernel,
        out_shape=made(UNIT, WIDTH),
        in_specs=[VMEM] * 8,
        out_specs=VMEM,
        scratch_shapes=[pltpu.VMEM((FOLD * UNIT, K), jnp.float32)],
        compiler_params=LIMIT,
        name="unit",
    )(*[near(p) for p in pieces])


def prepare_kernel(where, primal, dual, right, left, sems):
    at = pl.multiple_of((where[1] * 2 + where[2]) * K, K)
    copies = []
    for t in range(8):
        rows, here = pl.ds(t * K, K), pl.ds(at, K)
        copies.append((dual.at[rows, here], right.at[t, :, pl.ds(0, K)]))
        copies.append((primal.at[rows, here], right.at[t, :, pl.ds(K, K)]))
        copies.append((primal.at[here, rows], left.at[t, :, pl.ds(0, K)]))
        copies.append((dual.at[here, rows], left.at[t, :, pl.ds(K, K)]))
    started = [pltpu.make_async_copy(a, b, sems.at[n]) for n, (a, b) in enumerate(copies)]
    for c in started:
        c.start()
    for c in started:
        c.wait()


def prepare_call(where, primal, dual):
    return pl.pallas_call(
        prepare_kernel,
        out_shape=[made(8, K, 2 * K)] * 2,
        in_specs=[SMEM, HBM, HBM],
        out_specs=[VMEM] * 2,
        scratch_shapes=[pltpu.SemaphoreType.DMA((32,))],
        compiler_params=LIMIT,
        name="prepare",
    )(where, far(primal), far(dual))


STRIDE = 40


def reduce_kernel(plan, chained, where, tiles, right, left, *refs):
    n = len(plan)
    blocks = refs[:n]
    out, *turns = refs[n + (1 if chained else 0) :]
    y, core = where[1], where[2]
    for b, (dy, dcore) in enumerate(plan):
        row = lax.rem(y + dy, 4) * 64 + lax.rem(core + dcore, 2) * 32
        turn = turns[b % 2]
        packed = len(blocks[b].shape) == 2
        if packed:
            ends = blocks[b][32 * H :, :].astype(jnp.float32)
        for m in range(32):
            t = tiles[row + m]
            if packed:
                kept = blocks[b][m * H : (m + 1) * H, :].astype(jnp.float32)
                square = unfolded(kept, ends[m : m + 1]).astype(jnp.bfloat16)
            else:
                square = blocks[b][m]
            wide = jnp.dot(square, right[t], preferred_element_type=jnp.float32)
            wide = wide.astype(jnp.bfloat16)
            tall = jnp.concatenate([wide[:, :K], wide[:, K:]], axis=0)
            both = jnp.dot(left[t], tall, preferred_element_type=jnp.float32)
            kept, last = folded(both, True)
            turn[pl.ds(m, H, stride=STRIDE), :] = kept
            turn[H * STRIDE + m : H * STRIDE + m + 1, :] = last
        rows = pl.ds(pl.multiple_of(row, 32), 32)
        for a in range(FOLD):
            part = turn[a * STRIDE : a * STRIDE + 32, :].astype(out.dtype)
            out[rows, a * K : (a + 1) * K] = part


def reduce_call(plan, where, tiles, blocks, right, left, total):
    n = len(blocks)
    args = [where, tiles, near(right), near(left), *[near(b) for b in blocks]]
    specs = [SMEM, SMEM, VMEM, VMEM] + [VMEM] * n
    aliases = {}
    if total is not None:
        aliases = {len(args): 0}
        args.append(near(total))
        specs.append(VMEM)
    return pl.pallas_call(
        functools.partial(reduce_kernel, plan, total is not None),
        out_shape=made(256, WIDTH),
        in_specs=specs,
        out_specs=VMEM,
        scratch_shapes=[
            pltpu.VMEM((FOLD * STRIDE, K), jnp.float32),
            pltpu.VMEM((FOLD * STRIDE, K), jnp.float32),
        ],
        input_output_aliases=aliases,
        compiler_params=LIMIT,
        name="reduced",
    )(*args)


def contract_kernel(n, *refs):
    units, total, outs = refs[:n], refs[n], refs[n + 1 :]
    rows = jnp.concatenate([u[...] for u in units], axis=0) if n > 1 else units[0][...]
    values = lax.dot_general(rows, total[...], NT, preferred_element_type=jnp.float32)
    for m in range(n):
        outs[m][...] = values[m * UNIT : (m + 1) * UNIT]


def contract_call(units, total):
    n = len(units)
    return pl.pallas_call(
        functools.partial(contract_kernel, n),
        out_shape=[made(UNIT, 256, dtype=jnp.float32)] * n,
        in_specs=[VMEM] * (n + 1),
        out_specs=[VMEM] * n,
        compiler_params=LIMIT,
        name="contract",
    )(*[near(u) for u in units], near(total))


def gather_kernel(known, where, *refs):
    n = len(known)
    values, outs, held = refs[:n], refs[n : n + 8], refs[n + 8]
    x, z, y, core = where[0] // 4, lax.rem(where[0], 4), where[1], where[2]
    for d, ref in zip(known, values):
        column, row = lax.rem(x - d[0] + 4, 4), lax.rem(z - d[1] + 4, 4)
        goal = lax.rem(column - y + 4, 4) * 2 + lax.rem(row // 2 + core, 2)
        held[goal * 2 + lax.rem(row, 2)] = ref[...]
    for k in range(8):
        outs[k][...] = held[2 * k : 2 * k + 2]


def gather_call(where, known):
    return pl.pallas_call(
        functools.partial(gather_kernel, tuple(known)),
        out_shape=[made(2, UNIT, 256, dtype=jnp.float32)] * 8,
        in_specs=[SMEM] + [VMEM] * len(known),
        out_specs=[VMEM] * 8,
        scratch_shapes=[pltpu.VMEM((16, UNIT, 256), jnp.float32)],
        compiler_params=LIMIT,
        name="gather",
    )(where, *[near(v) for v in known.values()])


FORMED_BITS = sum(1 << (d[0] * 4 + d[1]) for d in FORMED)


def straight_of(where, g):
    x, z = where[0] // 4, lax.rem(where[0], 4)
    goal = (where[1] * 2 + where[2]) * 2 + g
    apart = lax.rem(x - goal // 4 + 4, 4) * 4 + lax.rem(z - lax.rem(goal, 4) + 4, 4)
    return goal, (FORMED_BITS >> apart) & 1


def places_kernel(where, ids_ref, hot_ref):
    line, y, core = where[0], where[1], where[2]
    goals = [straight_of(where, g) for g in range(2)]
    lines = [jnp.where(straight > 0, goal, line) for goal, straight in goals]
    pairs = [ids_ref[pl.ds(2 * n, 2), :] for n in lines]
    ids = jnp.concatenate(pairs + pairs, axis=0)
    lane = lax.broadcasted_iota(jnp.int32, (8, K), 1)
    half = lax.broadcasted_iota(jnp.int32, (8, K), 0) % 2
    ordinal = jnp.zeros((8, K), jnp.int32)
    for s in range(1, 32):
        same = jnp.logical_and(pltpu.roll(ids, s, 1) == ids, (lane & 31) >= s)
        ordinal = ordinal + same.astype(jnp.int32)
    block = half * 4 + (lane >> 5)
    step = ((ids >> 1) - (block >> 1)) & 3
    source = ((y - (ids >> 1)) & 3) * 2 + ((ids + core) & 1)
    place = source * UNIT + step * (2 * MOST) + ((ids + block) & 1) * MOST + ordinal
    columns = place.T
    slots = lax.broadcasted_iota(jnp.int32, (256, 8 * UNIT), 1)
    for g in range(2):
        chosen = jnp.concatenate(
            [columns[:, 2 * g : 2 * g + 1], columns[:, 2 * g + 1 : 2 * g + 2]], axis=0
        )
        hot_ref[g] = (slots == chosen).astype(hot_ref.dtype)


def places_call(where, ids):
    return pl.pallas_call(
        places_kernel,
        out_shape=made(2, 256, 8 * UNIT),
        in_specs=[SMEM, VMEM],
        out_specs=VMEM,
        compiler_params=LIMIT,
        name="places",
    )(where, ids)


def final_kernel(where, hot_ref, *refs):
    landed, out, held, sems = refs[:8], *refs[8:]
    stores = []
    for g in range(2):
        _, straight = straight_of(where, g)
        values = jnp.concatenate([ref[g] for ref in landed], axis=0)
        high = values.astype(jnp.bfloat16)
        low = (values - high.astype(jnp.float32)).astype(jnp.bfloat16)
        hot = hot_ref[g]
        picked = jnp.dot(hot, high, preferred_element_type=jnp.float32)
        picked = picked + jnp.dot(hot, low, preferred_element_type=jnp.float32)

        @pl.when(straight == 0)
        def _():
            held[g] = picked

        @pl.when(straight > 0)
        def _():
            held[g] = picked.T

        store = pltpu.make_async_copy(held.at[g], out.at[:, pl.ds(g * 256, 256)], sems.at[g])
        store.start()
        stores.append(store)
    for store in stores:
        store.wait()


def final_call(where, hot, landed):
    return pl.pallas_call(
        final_kernel,
        out_shape=jax.ShapeDtypeStruct((256, 512), jnp.float32),
        in_specs=[SMEM] + [VMEM] * 9,
        out_specs=HBM,
        scratch_shapes=[
            pltpu.VMEM((2, 256, 256), jnp.float32),
            pltpu.SemaphoreType.DMA((2,)),
        ],
        compiler_params=LIMIT,
        name="final",
    )(where, near(hot), *[near(v) for v in landed])


def steps(coeffs, tiles, primal, dual_inverse):
    x, z = lax.axis_index("x"), lax.axis_index("z")
    y, core = lax.axis_index("y"), lax.axis_index("core")
    line = x * 4 + z
    where = jnp.stack([line, y, core]).astype(jnp.int32)
    flat = tiles.reshape(4096)
    line_ids = lax.dynamic_slice_in_dim(flat, line * 256, 256, 0)

    *pieces, plain = fold_call(where, flat, coeffs)
    routed = [pieces[0]]
    for k in range(1, 8):
        routed.append(line_shift(pieces[k], k // 2, k % 2))
    units = {(0, 0): unit_call(routed)}
    right, left = prepare_call(where, primal, dual_inverse)

    other = line_shift(coeffs, 0, 1)
    down = line_shift(plain, 1, 0)
    up = line_shift(plain, 3, 0)
    across = line_shift(plain, 2, 0)
    down_other = line_shift(down, 0, 1)
    up_other = line_shift(up, 0, 1)
    across_other = line_shift(across, 0, 1)

    def formed(plan, blocks, total):
        return reduce_call(plan, where, line_ids, blocks, right, left, total)

    total = formed(((0, 0), (0, 1)), [coeffs, other], None)
    total = formed(((3, 0), (3, 1)), [down, down_other], total)
    total = formed(((1, 0), (1, 1)), [up, up_other], total)
    total = formed(((2, 0), (2, 1)), [across, across_other], total)

    for d, parent in FIRST + SECOND + THIRD:
        shift = ((d[0] - parent[0]) % 4, (d[1] - parent[1]) % 4)
        units[d] = plane_shift(units[parent], shift)

    known = {}
    for part in (EARLY, MIDDLE, LATE):
        values = contract_call([units[d] for d in part], total)
        known.update(zip(part, values))
    for d in EARLY + MIDDLE:
        if negated(d) in TURNED:
            known[negated(d)] = plane_shift(known[d], negated(d))
    ordered = gather_call(where, known)
    landed = [ordered[0]]
    for k in range(1, 8):
        landed.append(line_shift(ordered[k], k // 2, k % 2))
    hot = places_call(where, tiles.reshape(32, K))
    return final_call(where, hot, landed)


def solution(mesh):
    finer = Mesh(mesh.devices.reshape(4, 4, 4, 2), ALL)
    in_specs = (P(ALL, None, None), P(), P(), P())
    out_specs = P(PLANE, LINE)
    return jax.shard_map(
        steps, mesh=finer, in_specs=in_specs, out_specs=out_specs, check_vma=False
    )
```

```python
import functools

import jax
import jax.numpy as jnp
from jax import lax
from jax.experimental import pallas as pl
from jax.experimental.pallas import tpu as pltpu
from jax.sharding import Mesh
from jax.sharding import PartitionSpec as P


MOST = 5
K = 128
H = 64
FOLD = H + 1
WIDTH = FOLD * K
UNIT = 8 * MOST
PIECE = MOST * H + 16
LINE = ("y", "core")
PLANE = ("x", "z")
ALL = ("x", "z", "y", "core")
NT = (((1,), (1,)), ((), ()))
VMEM = pl.BlockSpec(memory_space=pltpu.VMEM)
SMEM = pl.BlockSpec(memory_space=pltpu.SMEM)
HBM = pl.BlockSpec(memory_space=pltpu.HBM)

LIMIT = pltpu.CompilerParams(vmem_limit_bytes=20 << 20)


def near(x):
    return pltpu.with_memory_space_constraint(x, pltpu.VMEM)


def far(x):
    return pltpu.with_memory_space_constraint(x, pltpu.HBM)


def made(*shape, dtype=jnp.bfloat16):
    return pltpu.VMEM(shape, dtype)


FIRST = (((1, 0), (0, 0)), ((0, 3), (0, 0)), ((3, 1), (0, 0)))
SECOND = (((3, 2), (3, 1)), ((2, 1), (3, 1)), ((2, 0), (1, 0)), ((0, 2), (0, 3)))
THIRD = (((1, 1), (1, 0)), ((2, 2), (3, 2)))
EARLY = ((0, 0), (1, 0), (0, 3), (3, 1), (3, 2), (2, 1))
MIDDLE = ((2, 0), (0, 2), (1, 1))
LATE = ((2, 2),)
FORMED = EARLY + MIDDLE + LATE


def negated(d):
    return ((-d[0]) % 4, (-d[1]) % 4)


TURNED = tuple(negated(d) for d in FORMED if negated(d) not in FORMED)


def plane_shift(x, shift):
    pairs = []
    for a in range(4):
        for b in range(4):
            pairs.append((a * 4 + b, (a + shift[0]) % 4 * 4 + (b + shift[1]) % 4))
    return lax.ppermute(x, PLANE, pairs)


def line_shift(x, shift, swap):
    pairs = []
    for a in range(4):
        for b in range(2):
            pairs.append((a * 2 + b, (a + shift) % 4 * 2 + (b + swap) % 2))
    return lax.ppermute(x, LINE, pairs)


def folded(square, half_diagonal):
    top, bottom = square[:H], square[H:]
    row = lax.broadcasted_iota(jnp.int32, (H, K), 0)
    lane = lax.broadcasted_iota(jnp.int32, (H, K), 1)
    turned = pltpu.roll(bottom, H, 1)
    kept = jnp.where(jnp.logical_and(lane < H, row > lane), turned, top)
    last = jnp.sum(jnp.where(lane == row + H, bottom, 0.0), axis=0, keepdims=True)
    if half_diagonal:
        kept = kept * jnp.where(row == lane, 0.5, 1.0)
        last = last * 0.5
    return kept, last


def unfolded(kept, last):
    row = lax.broadcasted_iota(jnp.int32, (H, K), 0)
    lane = lax.broadcasted_iota(jnp.int32, (H, K), 1)
    wide = jnp.concatenate([kept, kept], axis=0).T
    head, tail = wide[:H], wide[H:]
    top = jnp.where(jnp.logical_and(lane < H, row > lane), head, kept)
    corner = pltpu.roll(jnp.where(row > lane, kept, head), H, 1)
    right = jnp.where(lane == row + H, last, corner)
    return jnp.concatenate([top, jnp.where(lane < H, tail, right)], axis=0)


def fold_kernel(where, tiles, own_ref, *refs):
    outs, plain, held, lasts, ends, counts, near_ref, sems = refs[:8], *refs[8:]
    loads = []
    for n in range(4):
        rows = pl.ds(n * 8, 8)
        loads.append(pltpu.make_async_copy(own_ref.at[rows], near_ref.at[rows], sems.at[n]))
        loads[n].start()
    held[...] = jnp.zeros(held.shape, held.dtype)
    lasts[...] = jnp.zeros(lasts.shape, lasts.dtype)
    for k in range(8):
        counts[k] = 0
    y, core = where[1], where[2]
    mine = where[0] * 256 + y * 64 + core * 32

    for n in range(4):
        loads[n].wait()
        for m in range(8):
            i = n * 8 + m
            t = tiles[mine + i]
            order = counts[t]
            counts[t] = order + 1
            goal = lax.rem(t // 2 - y + 4, 4) * 2 + lax.rem(t + core, 2)
            kept, last = folded(near_ref[i].astype(jnp.float32), False)
            row = pl.multiple_of(goal * PIECE + order * H, 16)
            kept = kept.astype(held.dtype)
            held[pl.ds(row, H), :] = kept
            plain[i * H : (i + 1) * H, :] = kept
            ends[i : i + 1, :] = last
            lasts[pl.ds(goal * 16 + order, 1), :] = last
    plain[32 * H :, :] = ends[...].astype(plain.dtype)
    for k in range(8):
        outs[k][: MOST * H, :] = held[k * PIECE : k * PIECE + MOST * H, :]
        outs[k][MOST * H :, :] = lasts[k * 16 : (k + 1) * 16, :].astype(held.dtype)


def fold_call(where, tiles, own):
    return pl.pallas_call(
        fold_kernel,
        out_shape=[made(PIECE, K)] * 8 + [made(32 * H + 32, K)],
        in_specs=[SMEM, SMEM, HBM],
        out_specs=[VMEM] * 9,
        scratch_shapes=[
            pltpu.VMEM((8 * PIECE, K), jnp.bfloat16),
            pltpu.VMEM((8 * 16, K), jnp.float32),
            pltpu.VMEM((32, K), jnp.float32),
            pltpu.SMEM((8,), jnp.int32),
            pltpu.VMEM((32, K, K), jnp.bfloat16),
            pltpu.SemaphoreType.DMA((4,)),
        ],
        compiler_params=LIMIT,
        name="fold",
    )(where, far(tiles), far(own))


def unit_kernel(*refs):
    pieces, out, turn = refs[:8], refs[8], refs[9]
    for k in range(8):
        for s in range(MOST):
            slot = k * MOST + s
            turn[pl.ds(slot, H, stride=UNIT), :] = pieces[k][s * H : (s + 1) * H, :].astype(jnp.float32)
        first = H * UNIT + k * MOST
        turn[first : first + MOST, :] = pieces[k][MOST * H :, :].astype(jnp.float32)[:MOST]
    for a in range(FOLD):
        out[:, a * K : (a + 1) * K] = turn[a * UNIT : (a + 1) * UNIT, :].astype(out.dtype)


def unit_call(pieces):
    return pl.pallas_call(
        unit_kernel,
        out_shape=made(UNIT, WIDTH),
        in_specs=[VMEM] * 8,
        out_specs=VMEM,
        scratch_shapes=[pltpu.VMEM((FOLD * UNIT, K), jnp.float32)],
        compiler_params=LIMIT,
        name="unit",
    )(*[near(p) for p in pieces])


def prepare_kernel(where, primal, dual, right, left, sems):
    at = pl.multiple_of((where[1] * 2 + where[2]) * K, K)
    copies = []
    for t in range(8):
        rows, here = pl.ds(t * K, K), pl.ds(at, K)
        copies.append((dual.at[rows, here], right.at[t, :, pl.ds(0, K)]))
        copies.append((primal.at[rows, here], right.at[t, :, pl.ds(K, K)]))
        copies.append((primal.at[here, rows], left.at[t, :, pl.ds(0, K)]))
        copies.append((dual.at[here, rows], left.at[t, :, pl.ds(K, K)]))
    started = [pltpu.make_async_copy(a, b, sems.at[n]) for n, (a, b) in enumerate(copies)]
    for c in started:
        c.start()
    for c in started:
        c.wait()


def prepare_call(where, primal, dual):
    return pl.pallas_call(
        prepare_kernel,
        out_shape=[made(8, K, 2 * K)] * 2,
        in_specs=[SMEM, HBM, HBM],
        out_specs=[VMEM] * 2,
        scratch_shapes=[pltpu.SemaphoreType.DMA((32,))],
        compiler_params=LIMIT,
        name="prepare",
    )(where, far(primal), far(dual))


STRIDE = 40


def reduce_kernel(plan, chained, where, tiles, right, left, *refs):
    n = len(plan)
    blocks = refs[:n]
    out, *turns = refs[n + (1 if chained else 0) :]
    y, core = where[1], where[2]
    for b, (dy, dcore) in enumerate(plan):
        row = lax.rem(y + dy, 4) * 64 + lax.rem(core + dcore, 2) * 32
        turn = turns[b % 2]
        packed = len(blocks[b].shape) == 2
        if packed:
            ends = blocks[b][32 * H :, :].astype(jnp.float32)
        for m in range(32):
            t = tiles[row + m]
            if packed:
                kept = blocks[b][m * H : (m + 1) * H, :].astype(jnp.float32)
                square = unfolded(kept, ends[m : m + 1]).astype(jnp.bfloat16)
            else:
                square = blocks[b][m]
            wide = jnp.dot(square, right[t], preferred_element_type=jnp.float32)
            wide = wide.astype(jnp.bfloat16)
            tall = jnp.concatenate([wide[:, :K], wide[:, K:]], axis=0)
            both = jnp.dot(left[t], tall, preferred_element_type=jnp.float32)
            kept, last = folded(both, True)
            turn[pl.ds(m, H, stride=STRIDE), :] = kept
            turn[H * STRIDE + m : H * STRIDE + m + 1, :] = last
        rows = pl.ds(pl.multiple_of(row, 32), 32)
        for a in range(FOLD):
            part = turn[a * STRIDE : a * STRIDE + 32, :].astype(out.dtype)
            out[rows, a * K : (a + 1) * K] = part


def reduce_call(plan, where, tiles, blocks, right, left, total):
    n = len(blocks)
    args = [where, tiles, near(right), near(left), *[near(b) for b in blocks]]
    specs = [SMEM, SMEM, VMEM, VMEM] + [VMEM] * n
    aliases = {}
    if total is not None:
        aliases = {len(args): 0}
        args.append(near(total))
        specs.append(VMEM)
    return pl.pallas_call(
        functools.partial(reduce_kernel, plan, total is not None),
        out_shape=made(256, WIDTH),
        in_specs=specs,
        out_specs=VMEM,
        scratch_shapes=[
            pltpu.VMEM((FOLD * STRIDE, K), jnp.float32),
            pltpu.VMEM((FOLD * STRIDE, K), jnp.float32),
        ],
        input_output_aliases=aliases,
        compiler_params=LIMIT,
        name="reduced",
    )(*args)


def contract_kernel(n, *refs):
    units, total, outs = refs[:n], refs[n], refs[n + 1 :]
    rows = jnp.concatenate([u[...] for u in units], axis=0) if n > 1 else units[0][...]
    values = lax.dot_general(rows, total[...], NT, preferred_element_type=jnp.float32)
    for m in range(n):
        outs[m][...] = values[m * UNIT : (m + 1) * UNIT]


def contract_call(units, total):
    n = len(units)
    return pl.pallas_call(
        functools.partial(contract_kernel, n),
        out_shape=[made(UNIT, 256, dtype=jnp.float32)] * n,
        in_specs=[VMEM] * (n + 1),
        out_specs=[VMEM] * n,
        compiler_params=LIMIT,
        name="contract",
    )(*[near(u) for u in units], near(total))


def gather_kernel(known, where, *refs):
    n = len(known)
    values, outs, held = refs[:n], refs[n : n + 8], refs[n + 8]
    x, z, y, core = where[0] // 4, lax.rem(where[0], 4), where[1], where[2]
    for d, ref in zip(known, values):
        column, row = lax.rem(x - d[0] + 4, 4), lax.rem(z - d[1] + 4, 4)
        goal = lax.rem(column - y + 4, 4) * 2 + lax.rem(row // 2 + core, 2)
        held[goal * 2 + lax.rem(row, 2)] = ref[...]
    for k in range(8):
        outs[k][...] = held[2 * k : 2 * k + 2]


def gather_call(where, known):
    return pl.pallas_call(
        functools.partial(gather_kernel, tuple(known)),
        out_shape=[made(2, UNIT, 256, dtype=jnp.float32)] * 8,
        in_specs=[SMEM] + [VMEM] * len(known),
        out_specs=[VMEM] * 8,
        scratch_shapes=[pltpu.VMEM((16, UNIT, 256), jnp.float32)],
        compiler_params=LIMIT,
        name="gather",
    )(where, *[near(v) for v in known.values()])


FORMED_BITS = sum(1 << (d[0] * 4 + d[1]) for d in FORMED)


def straight_of(where, g):
    x, z = where[0] // 4, lax.rem(where[0], 4)
    goal = (where[1] * 2 + where[2]) * 2 + g
    apart = lax.rem(x - goal // 4 + 4, 4) * 4 + lax.rem(z - lax.rem(goal, 4) + 4, 4)
    return goal, (FORMED_BITS >> apart) & 1


def places_kernel(where, ids_ref, hot_ref):
    line, y, core = where[0], where[1], where[2]
    goals = [straight_of(where, g) for g in range(2)]
    lines = [jnp.where(straight > 0, goal, line) for goal, straight in goals]
    pairs = [ids_ref[pl.ds(2 * n, 2), :] for n in lines]
    ids = jnp.concatenate(pairs + pairs, axis=0)
    lane = lax.broadcasted_iota(jnp.int32, (8, K), 1)
    half = lax.broadcasted_iota(jnp.int32, (8, K), 0) % 2
    ordinal = jnp.zeros((8, K), jnp.int32)
    for s in range(1, 32):
        same = jnp.logical_and(pltpu.roll(ids, s, 1) == ids, (lane & 31) >= s)
        ordinal = ordinal + same.astype(jnp.int32)
    block = half * 4 + (lane >> 5)
    step = ((ids >> 1) - (block >> 1)) & 3
    source = ((y - (ids >> 1)) & 3) * 2 + ((ids + core) & 1)
    place = source * UNIT + step * (2 * MOST) + ((ids + block) & 1) * MOST + ordinal
    columns = place.T
    slots = lax.broadcasted_iota(jnp.int32, (256, 8 * UNIT), 1)
    for g in range(2):
        chosen = jnp.concatenate(
            [columns[:, 2 * g : 2 * g + 1], columns[:, 2 * g + 1 : 2 * g + 2]], axis=0
        )
        hot_ref[g] = (slots == chosen).astype(hot_ref.dtype)


def places_call(where, ids):
    return pl.pallas_call(
        places_kernel,
        out_shape=made(2, 256, 8 * UNIT),
        in_specs=[SMEM, VMEM],
        out_specs=VMEM,
        compiler_params=LIMIT,
        name="places",
    )(where, ids)


def final_kernel(where, hot_ref, *refs):
    landed, out, held, sems = refs[:8], *refs[8:]
    stores = []
    for g in range(2):
        _, straight = straight_of(where, g)
        values = jnp.concatenate([ref[g] for ref in landed], axis=0)
        high = values.astype(jnp.bfloat16)
        low = (values - high.astype(jnp.float32)).astype(jnp.bfloat16)
        hot = hot_ref[g]
        picked = jnp.dot(hot, high, preferred_element_type=jnp.float32)
        picked = picked + jnp.dot(hot, low, preferred_element_type=jnp.float32)

        @pl.when(straight == 0)
        def _():
            held[g] = picked

        @pl.when(straight > 0)
        def _():
            held[g] = picked.T

        store = pltpu.make_async_copy(held.at[g], out.at[:, pl.ds(g * 256, 256)], sems.at[g])
        store.start()
        stores.append(store)
    for store in stores:
        store.wait()


def final_call(where, hot, landed):
    return pl.pallas_call(
        final_kernel,
        out_shape=jax.ShapeDtypeStruct((256, 512), jnp.float32),
        in_specs=[SMEM] + [VMEM] * 9,
        out_specs=HBM,
        scratch_shapes=[
            pltpu.VMEM((2, 256, 256), jnp.float32),
            pltpu.SemaphoreType.DMA((2,)),
        ],
        compiler_params=LIMIT,
        name="final",
    )(where, near(hot), *[near(v) for v in landed])


def steps(coeffs, tiles, primal, dual_inverse):
    x, z = lax.axis_index("x"), lax.axis_index("z")
    y, core = lax.axis_index("y"), lax.axis_index("core")
    line = x * 4 + z
    where = jnp.stack([line, y, core]).astype(jnp.int32)
    flat = tiles.reshape(4096)
    line_ids = lax.dynamic_slice_in_dim(flat, line * 256, 256, 0)

    *pieces, plain = fold_call(where, flat, coeffs)
    routed = [pieces[0]]
    for k in range(1, 8):
        routed.append(line_shift(pieces[k], k // 2, k % 2))
    units = {(0, 0): unit_call(routed)}
    right, left = prepare_call(where, primal, dual_inverse)

    other = line_shift(coeffs, 0, 1)
    down = line_shift(plain, 1, 0)
    up = line_shift(plain, 3, 0)
    across = line_shift(plain, 2, 0)
    down_other = line_shift(down, 0, 1)
    up_other = line_shift(up, 0, 1)
    across_other = line_shift(across, 0, 1)

    def formed(plan, blocks, total):
        return reduce_call(plan, where, line_ids, blocks, right, left, total)

    total = formed(((0, 0), (0, 1)), [coeffs, other], None)
    total = formed(((3, 0), (3, 1)), [down, down_other], total)
    total = formed(((1, 0), (1, 1)), [up, up_other], total)
    total = formed(((2, 0), (2, 1)), [across, across_other], total)

    for d, parent in FIRST + SECOND + THIRD:
        shift = ((d[0] - parent[0]) % 4, (d[1] - parent[1]) % 4)
        units[d] = plane_shift(units[parent], shift)

    known = {}
    for part in (EARLY, MIDDLE, LATE):
        values = contract_call([units[d] for d in part], total)
        known.update(zip(part, values))
    for d in EARLY + MIDDLE[2:]:
        if negated(d) in TURNED:
            known[negated(d)] = plane_shift(known[d], negated(d))
    ordered = gather_call(where, known)
    landed = [ordered[0]]
    for k in range(1, 8):
        landed.append(line_shift(ordered[k], k // 2, k % 2))
    hot = places_call(where, tiles.reshape(32, K))
    return final_call(where, hot, landed)


def solution(mesh):
    finer = Mesh(mesh.devices.reshape(4, 4, 4, 2), ALL)
    in_specs = (P(ALL, None, None), P(), P(), P())
    out_specs = P(PLANE, LINE)
    return jax.shard_map(
        steps, mesh=finer, in_specs=in_specs, out_specs=out_specs, check_vma=False
    )
```
